256 devices in a mesh: client: 16 (over z_hi, x, core), tp: 16 (over y, z_lo).
Axes of the slice: x: 4, y: 4, z: 8 (z_hi: 2, z_lo: 4; z = z_hi * 4 + z_lo), core: 2. Of those that a mesh axis runs over, the one named last changes fastest.
Arguments:
- inputs: bfloat16 [16, 128, 2048], P('client'), may hold values from -6 to 6
- targets: bfloat16 [16, 128, 2048], P('client'), may hold values from -6 to 6
- norm_gain: float32 [2048], replicated, may hold values from 0.1 to 1.9
- gate_weight: bfloat16 [2048, 4096], P(None, 'tp'), may hold values from -0.125 to 0.125
- up_weight: bfloat16 [2048, 4096], P(None, 'tp'), may hold values from -0.125 to 0.125
- down_weight: bfloat16 [4096, 2048], P('tp'), may hold values from -0.09375 to 0.09375
- overflow: int32 [16, 3, 16], P('client', None, 'tp'), may hold values 0 or 1
Outputs:
- gate_update: float32 [2048, 4096], P('client', 'tp')
- up_update: float32 [2048, 4096], P('client', 'tp')
- down_update: float32 [4096, 2048], P('tp', 'client')
- gain_update: float32 [2048], P('client')
The draws below stay inside these ranges and needn't reach their ends.
All inputs are finite; a program needn't handle non-finite values. No bound on the sum of `overflow` on one device may be relied on, other than what follows from the above.
Results may differ from the reference program's by a relative error of at most 0.014.
Values may be sent and summed in bfloat16 or wider, within the bound.
No kernel may reach another device: no remote copies, remote signals or barrier semaphores. Data moves between devices by JAX's collectives and lax.ppermute only.
A program may use at most 64 MiB of HBM per device.

```python
import math
import jax
import jax.numpy as jnp
from jax import lax

D = 2048
FF = 4096
TOK_DEV = 128
STEPS = 3
CLIENTS = 16
N_TP = 16


def set_ends(drawn, own_key, low, high):
    shape = drawn.shape
    place = [jax.random.randint(jax.random.fold_in(own_key, axis), (), 0, shape[axis]) for axis in range(len(shape))]
    drawn = drawn.at[tuple(place)].set(low)
    longest = shape.index(max(shape))
    place[longest] = (place[longest] + 1) % shape[longest]
    return drawn.at[tuple(place)].set(high)


def level_of(own_key, dims, shards, low, largest):
    loudness, own = 1.0, jax.random.fold_in(own_key, 6)
    for dim, blocks in shards:
        draws = jnp.exp(jax.random.uniform(jax.random.fold_in(own, dim), (blocks,), jnp.float32, low / len(shards), largest / len(shards)))
        loudness = loudness * jnp.repeat(draws, dims[dim] // blocks).reshape([-1 if axis == dim else 1 for axis in range(len(dims))])
    return loudness


def normal_values(own_key, extent, scale, reach, split=(), dtype=jnp.bfloat16):
    result = jax.random.normal(own_key, extent, jnp.float32) * scale
    if len(split) > 0:
        result = level_of(own_key, extent, split, -0.22, 0.18) * result
    return jnp.clip(result, min=-reach, max=reach).astype(dtype)


def setup_inputs(seed: int = 0) -> dict:
    arg_keys = jax.random.split(jax.random.key(seed), 8)
    return {
        "inputs": normal_values(arg_keys[0], (CLIENTS, TOK_DEV, D), 1.0, 6.0, ((0, 16),)),
        "targets": normal_values(arg_keys[1], (CLIENTS, TOK_DEV, D), 1.0, 6.0, ((0, 16),)),
        "norm_gain": jnp.clip(1.0 + 0.18 * jax.random.normal(arg_keys[2], (D,), jnp.float32), 0.1, 1.9),
        "gate_weight": normal_values(arg_keys[3], (D, FF), D ** -0.5, 0.125, ((1, 16),)),
        "up_weight": normal_values(arg_keys[4], (D, FF), D ** -0.5, 0.125, ((1, 16),)),
        "down_weight": normal_values(arg_keys[5], (FF, D), FF ** -0.5, 0.09375, ((0, 16),)),
        "overflow": set_ends((jax.random.randint(arg_keys[6], (CLIENTS, STEPS, N_TP), 0, 64) < 1).astype(jnp.int32), jax.random.fold_in(arg_keys[6], 1), 0, 1),
    }


def client_round(features, target_rows, flag_rows, norm_gain, gate_weight, up_weight, down_weight):
    limit = 0.5 * math.sqrt(3.0 * D * FF)
    activ = features.astype(jnp.float32)
    scaled = activ * lax.rsqrt(lax.optimization_barrier(jnp.mean(activ * activ, axis=-1, keepdims=True)) + 1e-05)
    gain_master = norm_gain.astype(jnp.float32)
    gate_master = gate_weight.astype(jnp.float32)
    up_master = up_weight.astype(jnp.float32)
    down_master = down_weight.astype(jnp.float32)
    gate_total = jnp.zeros_like(gate_master)
    up_total = jnp.zeros_like(up_master)
    down_total = jnp.zeros_like(down_master)
    gain_total = jnp.zeros_like(gain_master)
    for local_step in range(STEPS):
        normed = (scaled * gain_master).astype(jnp.bfloat16)
        gate_copy = gate_master.astype(jnp.bfloat16)
        up_copy = up_master.astype(jnp.bfloat16)
        down_copy = down_master.astype(jnp.bfloat16)
        gate_act = jnp.dot(normed, gate_copy, preferred_element_type=jnp.float32)
        up_act = jnp.dot(normed, up_copy, preferred_element_type=jnp.float32)
        sig_gate = jax.nn.sigmoid(gate_act)
        silu_gate = gate_act * sig_gate
        hidden = (silu_gate * up_act).astype(jnp.bfloat16)
        outputs = activ + jnp.dot(hidden, down_copy, preferred_element_type=jnp.float32)
        grad_out = (outputs - target_rows.astype(jnp.float32)).astype(jnp.bfloat16)
        grad_down = jnp.dot(hidden.T, grad_out, preferred_element_type=jnp.float32)
        grad_hidden = jnp.dot(grad_out, down_copy.T, preferred_element_type=jnp.float32)
        grad_gate_act = (grad_hidden * up_act * (sig_gate * (1.0 + gate_act * (1.0 - sig_gate)))).astype(jnp.bfloat16)
        grad_up_act = (grad_hidden * silu_gate).astype(jnp.bfloat16)
        grad_gate = jnp.dot(normed.T, grad_gate_act, preferred_element_type=jnp.float32)
        grad_up = jnp.dot(normed.T, grad_up_act, preferred_element_type=jnp.float32)
        grad_normed = jnp.dot(grad_gate_act, gate_copy.T, preferred_element_type=jnp.float32)
        grad_normed = grad_normed + jnp.dot(grad_up_act, up_copy.T, preferred_element_type=jnp.float32)
        grad_gain = lax.optimization_barrier(jnp.sum(grad_normed * scaled, axis=0))
        squares = jnp.sum(grad_gate * grad_gate) + jnp.sum(grad_up * grad_up) + jnp.sum(grad_down * grad_down)
        squares = squares + jnp.sum(grad_gain * grad_gain)
        grad_norm = jnp.sqrt(squares + 1e-06)
        flagged = jnp.sum(flag_rows[local_step])
        factor = jnp.where(flagged == 0, limit / jnp.maximum(grad_norm, limit), 0.0)
        gate_master = gate_master - 0.005 * factor * grad_gate
        up_master = up_master - 0.005 * factor * grad_up
        down_master = down_master - 0.005 * factor * grad_down
        gain_master = gain_master - 0.005 * factor * grad_gain
        gate_total = gate_total + factor * grad_gate
        up_total = up_total + factor * grad_up
        down_total = down_total + factor * grad_down
        gain_total = gain_total + factor * grad_gain
    return (gate_total, up_total, down_total, gain_total)

def reference(inputs, targets, norm_gain, gate_weight, up_weight, down_weight, overflow):

    def visit(carry, items):
        features, target_rows, flag_rows = items
        totals = client_round(features, target_rows, flag_rows, norm_gain, gate_weight, up_weight, down_weight)
        return (tuple((a + b for a, b in zip(carry, totals))), None)
    start = (jnp.zeros((D, FF), jnp.float32), jnp.zeros((D, FF), jnp.float32), jnp.zeros((FF, D), jnp.float32), jnp.zeros((D,), jnp.float32))
    sums, unused = lax.scan(visit, start, (inputs, targets, overflow))
    return (sums[0] / CLIENTS, sums[1] / CLIENTS, sums[2] / CLIENTS, sums[3] / CLIENTS)
```

```python
import math

import jax
import jax.numpy as jnp
from jax import lax
from jax.sharding import PartitionSpec as P

D = 2048
FF = 4096
STEPS = 3
RATE = 0.005


BF16 = jnp.bfloat16
F32 = jnp.float32


def dot_nn(a, b):
    return jnp.dot(a, b, preferred_element_type=F32)


def dot_nt(a, b):
    return lax.dot_general(a, b, (((1,), (1,)), ((), ())), preferred_element_type=F32)


def dot_tn(a, b):
    return lax.dot_general(a, b, (((0,), (0,)), ((), ())), preferred_element_type=F32)


def pieces(value):
    first = lax.reduce_precision(value, 8, 7)
    rest = value - first
    second = lax.reduce_precision(rest, 8, 7)
    third = rest - second
    return [first.astype(BF16), second.astype(BF16), third.astype(BF16)]


def client_perm(dh, dx, dc):
    return [
        (h * 8 + x * 2 + c, ((h + dh) % 2) * 8 + ((x + dx) % 4) * 2 + (c + dc) % 2)
        for h in range(2)
        for x in range(4)
        for c in range(2)
    ]


def small_sums(gain_part, square_part, flag_part):
    head = gain_part.astype(BF16).reshape(1, D)
    tail = jnp.stack(pieces(square_part) + [flag_part.astype(BF16)]).reshape(1, 4)
    tail = jnp.pad(tail, ((0, 0), (0, 124)))
    packed = jnp.concatenate([head, tail], axis=1)
    packed = jnp.broadcast_to(packed[None], (16, 1, D + 128))
    arrived = lax.all_to_all(packed, "tp", 0, 0, tiled=True)
    sums = jnp.sum(arrived.astype(F32), axis=(0, 1))
    return sums[:D], sums[D] + sums[D + 1] + sums[D + 2], sums[D + 3]


def on_device(inputs, targets, norm_gain, gate_weight, up_weight, down_weight, overflow):
    limit = 0.5 * math.sqrt(3.0 * D * FF)
    activ = inputs[0].astype(F32)
    scaled = activ * lax.rsqrt(jnp.mean(activ * activ, axis=-1, keepdims=True) + 1e-05)
    first_row = lax.axis_index("tp") * 8
    own_activ = lax.dynamic_slice_in_dim(inputs[0], first_row, 8, 0).astype(F32)
    own_target = lax.dynamic_slice_in_dim(targets[0], first_row, 8, 0).astype(F32)
    gain = norm_gain
    gain_total = jnp.zeros_like(gain)
    past = []
    for step in range(STEPS):
        normed = (scaled * gain).astype(BF16)
        gate_act = dot_nn(normed, gate_weight)
        up_act = dot_nn(normed, up_weight)
        for n, gg, gu, h, e, f in past:
            k = (dot_nt(normed, n) * (-RATE * f)).astype(BF16)
            gate_act = gate_act + dot_nn(k, gg)
            up_act = up_act + dot_nn(k, gu)
        sig = jax.nn.sigmoid(gate_act)
        silu = gate_act * sig
        hidden = (silu * up_act).astype(BF16)
        partial = dot_nn(hidden, down_weight)
        for n, gg, gu, h, e, f in past:
            k = (dot_nt(hidden, h) * (-RATE * f)).astype(BF16)
            partial = partial + dot_nn(k, e)
        arrived = lax.all_to_all(partial.astype(BF16).reshape(16, 8, D), "tp", 0, 0, tiled=True)
        outputs = own_activ + jnp.sum(arrived.astype(F32), axis=0)
        own_error = (outputs - own_target).astype(BF16)
        copies = jnp.broadcast_to(own_error[None], (16, 8, D))
        error = lax.all_to_all(copies, "tp", 0, 0, tiled=True).reshape(128, D)
        grad_hidden = dot_nt(error, down_weight)
        for n, gg, gu, h, e, f in past:
            k = (dot_nt(error, e) * (-RATE * f)).astype(BF16)
            grad_hidden = grad_hidden + dot_nn(k, h)
        g_gate = (grad_hidden * up_act * (sig * (1.0 + gate_act * (1.0 - sig)))).astype(BF16)
        g_up = (grad_hidden * silu).astype(BF16)
        grad_normed = dot_nt(g_gate, gate_weight) + dot_nt(g_up, up_weight)
        for n, gg, gu, h, e, f in past:
            k = ((dot_nt(g_gate, gg) + dot_nt(g_up, gu)) * (-RATE * f)).astype(BF16)
            grad_normed = grad_normed + dot_nn(k, n)
        gain_part = jnp.sum(grad_normed * scaled, axis=0)
        square_part = jnp.sum(dot_nt(normed, normed) * (dot_nt(g_gate, g_gate) + dot_nt(g_up, g_up)))
        square_part = square_part + jnp.sum(dot_nt(error, error) * dot_nt(hidden, hidden))
        flag_part = overflow[0, step, 0].astype(F32)
        grad_gain, squares, flagged = small_sums(gain_part, square_part, flag_part)
        grad_norm = jnp.sqrt(squares + jnp.sum(grad_gain * grad_gain) + 1e-06)
        factor = jnp.where(flagged < 0.5, limit / jnp.maximum(grad_norm, limit), 0.0)
        gain = gain - RATE * factor * grad_gain
        gain_total = gain_total + factor * grad_gain
        past.append((normed, g_gate, g_up, hidden, error, factor))

    me = lax.axis_index("client")
    core, x, hi = me % 2, (me // 2) % 4, me // 8

    gain_parts = gain_total.astype(BF16).reshape(16, 1, 128)
    gain_sum = jnp.sum(lax.all_to_all(gain_parts, "client", 0, 0, tiled=True).astype(F32), axis=(0, 1))

    left = jnp.concatenate([p[0] for p in past], axis=0).reshape(384, 8, 2, 128)
    error_all = jnp.concatenate([p[4] for p in past], axis=0).reshape(384, 8, 2, 128)
    grads = jnp.concatenate(
        [jnp.concatenate([(p[1].astype(F32) * p[5]).astype(BF16), (p[2].astype(F32) * p[5]).astype(BF16)], axis=1) for p in past],
        axis=0,
    )
    hid = jnp.concatenate([(p[3].astype(F32) * p[5]).astype(BF16) for p in past], axis=0)

    def totals(which):
        n = lax.dynamic_index_in_dim(left, which, 2, keepdims=False).reshape(384, 1024)
        e = lax.dynamic_index_in_dim(error_all, which, 2, keepdims=False).reshape(384, 1024)
        both = jnp.concatenate([dot_tn(n, grads).astype(BF16), dot_tn(e, hid).astype(BF16)], axis=1)
        return both.reshape(2, 4, 128, 768)

    other = totals(1 - core)
    swapped = lax.ppermute(other, "client", client_perm(0, 0, 1))
    pair = (totals(core).astype(F32) + swapped.astype(F32)).astype(BF16)
    line = lax.dynamic_index_in_dim(pair, x, 1, keepdims=False).astype(F32)
    for d in (2, 1, 3):
        out = lax.dynamic_index_in_dim(pair, (x + d) % 4, 1, keepdims=False)
        line = line + lax.ppermute(out, "client", client_perm(0, d, 0)).astype(F32)
    far = lax.dynamic_index_in_dim(line, 1 - hi, 0, keepdims=False).astype(BF16)
    near = lax.dynamic_index_in_dim(line, hi, 0, keepdims=False)
    full = (near + lax.ppermute(far, "client", client_perm(1, 0, 0)).astype(F32)) / 16
    return full[:, :256], full[:, 256:512], full[:, 512:].T, gain_sum / 16


def solution(mesh):
    placed = (
        P("client", None, None),
        P("client", None, None),
        P(),
        P(None, "tp"),
        P(None, "tp"),
        P("tp", None),
        P("client", None, "tp"),
    )
    return jax.shard_map(
        on_device,
        mesh=mesh,
        in_specs=placed,
        out_specs=(P("client", "tp"), P("client", "tp"), P("tp", "client"), P("client")),
        check_vma=False,
    )
```

```python
import math

import jax
import jax.numpy as jnp
from jax import lax
from jax.experimental import pallas as pl
from jax.experimental.pallas import tpu as pltpu
from jax.sharding import PartitionSpec as P

D = 2048
FF = 4096
STEPS = 3
RATE = 0.005
LIMIT = 0.5 * math.sqrt(3.0 * D * FF)
TOK = 128
UNITS = 256
ROWS = 3 * UNITS + 16


BF16 = jnp.bfloat16
F32 = jnp.float32


def dot_nn(a, b):
    return jnp.dot(a, b, preferred_element_type=F32)


def dot_nt(a, b):
    return lax.dot_general(a, b, (((1,), (1,)), ((), ())), preferred_element_type=F32)


def call(body, outs, args, scalars=()):
    return pl.pallas_call(
        body,
        out_shape=tuple(jax.ShapeDtypeStruct(s, d) for s, d in outs),
        in_specs=[pl.BlockSpec(memory_space=pltpu.SMEM)] * len(scalars)
        + [pl.BlockSpec(memory_space=pltpu.VMEM)] * len(args),
        out_specs=tuple(pl.BlockSpec(memory_space=pltpu.VMEM) for _ in outs),
        compiler_params=pltpu.CompilerParams(vmem_limit_bytes=24 * 1024 * 1024),
    )(*scalars, *args)


def forward(normed, wg, wu, down, past, coefs, act_ref, hid_ref, part_ref):
    gate = dot_nn(normed, wg[...])
    up = dot_nn(normed, wu[...])
    for (n, g, h, e), a in zip(past, coefs):
        k = (dot_nt(normed, n[...]) * a).astype(BF16)
        gate = gate - dot_nn(k, g[:, :UNITS])
        up = up - dot_nn(k, g[:, UNITS:])
    act_ref[:, :UNITS] = gate
    act_ref[:, UNITS:] = up
    hidden = (gate * jax.nn.sigmoid(gate) * up).astype(BF16)
    hid_ref[...] = hidden
    share = dot_nn(hidden, down[...])
    for (n, g, h, e), a in zip(past, coefs):
        k = (dot_nt(hidden, h[...]) * a).astype(BF16)
        share = share - dot_nn(k, e[...])
    part_ref[...] = share.astype(BF16).reshape(16, 8, D)


def first_body(x, gain, wg, wu, down, scaled_ref, norm_ref, act_ref, hid_ref, part_ref):
    activ = x[...].astype(F32)
    scaled = activ * lax.rsqrt(jnp.mean(activ * activ, axis=-1, keepdims=True) + 1e-05)
    scaled_ref[...] = scaled
    normed = (scaled * gain[...]).astype(BF16)
    norm_ref[...] = normed
    forward(normed, wg, wu, down, (), (), act_ref, hid_ref, part_ref)


def sums_of(arrived):
    total = arrived[0].astype(F32)
    for i in range(1, 16):
        total = total + arrived[i].astype(F32)
    grad_gain = jnp.concatenate([total[r : r + 1, :256] for r in range(8)], axis=1)
    squares = jnp.sum(jnp.sum(total[0:3, 256:], axis=0, keepdims=True), axis=1, keepdims=True)
    squares = squares + jnp.sum(grad_gain * grad_gain, axis=1, keepdims=True)
    flagged = total[3:4, 256:257]
    norm = jnp.sqrt(squares + 1e-06)
    factor = jnp.where(flagged < 0.5, LIMIT / jnp.maximum(norm, LIMIT), 0.0)
    return grad_gain, factor


def next_body(step, *refs):
    arrived, gain, gain_total, scaled, wg, wu, down = refs[:7]
    at = 7
    past = [refs[at + 4 * j : at + 4 * j + 4] for j in range(step)]
    at += 4 * step
    old = refs[at : at + step - 1]
    at += step - 1
    factor_ref, gain_ref, total_ref, norm_ref, act_ref, hid_ref, part_ref = refs[at:]
    grad_gain, factor = sums_of(arrived)
    factor_ref[...] = jnp.broadcast_to(factor, (8, 128))
    new_gain = gain[...] - RATE * factor * grad_gain
    gain_ref[...] = new_gain
    total_ref[...] = gain_total[...] + factor * grad_gain
    normed = (scaled[...] * new_gain).astype(BF16)
    norm_ref[...] = normed
    coefs = [RATE * r[0:1, 0:1] for r in old] + [RATE * factor]
    forward(normed, wg, wu, down, past, coefs, act_ref, hid_ref, part_ref)


def error_body(arrived, own_x, own_t, out_ref):
    total = arrived[0].astype(F32)
    for i in range(1, 16):
        total = total + arrived[i].astype(F32)
    error = (own_x[...].astype(F32) + total - own_t[...].astype(F32)).astype(BF16)
    for i in range(16):
        out_ref[i] = error


def pieces(value):
    first = value.astype(BF16)
    rest = value - first.astype(F32)
    second = rest.astype(BF16)
    third = (rest - second.astype(F32)).astype(BF16)
    return [first.astype(F32), second.astype(F32), third.astype(F32)]


def back_body(step, flags, *refs):
    error, wg, wu, down, scaled, normed, act, hidden = refs[:8]
    at = 8
    past = [refs[at + 4 * j : at + 4 * j + 4] for j in range(step)]
    at += 4 * step
    coefs = [RATE * r[0:1, 0:1] for r in refs[at : at + step]]
    at += step
    grad_ref, pay_ref = refs[at:]
    err = error[...].reshape(TOK, D)
    hid = hidden[...]
    nrm = normed[...]
    grad_hidden = dot_nt(err, down[...])
    for (n, g, h, e), a in zip(past, coefs):
        k = (dot_nt(err, e[...]) * a).astype(BF16)
        grad_hidden = grad_hidden - dot_nn(k, h[...])
    gate, up = act[:, :UNITS], act[:, UNITS:]
    sig = jax.nn.sigmoid(gate)
    g_gate = (grad_hidden * up * (sig * (1.0 + gate * (1.0 - sig)))).astype(BF16)
    g_up = (grad_hidden * (gate * sig)).astype(BF16)
    grad_ref[:, :UNITS] = g_gate
    grad_ref[:, UNITS:] = g_up
    grads = jnp.concatenate([g_gate, g_up], axis=1)
    grad_normed = dot_nt(g_gate, wg[...]) + dot_nt(g_up, wu[...])
    for (n, g, h, e), a in zip(past, coefs):
        k = (dot_nt(grads, g[...]) * a).astype(BF16)
        grad_normed = grad_normed - dot_nn(k, n[...])
    gain_part = jnp.sum(grad_normed * scaled[...], axis=0, keepdims=True)
    square = dot_nt(nrm, nrm) * dot_nt(grads, grads) + dot_nt(err, err) * dot_nt(hid, hid)
    square = jnp.sum(square, axis=0, keepdims=True)
    flag = jnp.full((1, 128), flags[step].astype(F32))
    tail = jnp.concatenate(pieces(square) + [flag, jnp.zeros((4, 128), F32)], axis=0)
    head = jnp.concatenate([gain_part[:, r * 256 : (r + 1) * 256] for r in range(8)], axis=0)
    packed = jnp.concatenate([head, tail], axis=1).astype(BF16)
    for i in range(16):
        pay_ref[i] = packed


def totals_body(which, *refs):
    arrived, gain_total = refs[:2]
    past = [refs[2 + 4 * j : 6 + 4 * j] for j in range(STEPS)]
    old = refs[2 + 4 * STEPS : 2 + 4 * STEPS + STEPS - 1]
    out_ref, left = refs[2 + 4 * STEPS + STEPS - 1 :]
    grad_gain, factor = sums_of(arrived)
    gains = gain_total[...] + factor * grad_gain
    factors = [r[0:1, 0:1] for r in old] + [factor]
    for j, ((n, g, h, e), f) in enumerate(zip(past, factors)):
        left[: 2 * UNITS, j * TOK : (j + 1) * TOK] = (g[...].astype(F32) * f).T.astype(BF16)
        left[2 * UNITS :, j * TOK : (j + 1) * TOK] = (h[...].astype(F32) * f).T.astype(BF16)
    w = which[0]
    for b in range(8):
        col = pl.ds(pl.multiple_of((2 * b + w) * 128, 128), 128)
        rows = jnp.concatenate([p[0][:, col] for p in past], axis=0)
        errs = jnp.concatenate([p[3][:, col] for p in past], axis=0)
        out_ref[b, : 2 * UNITS] = dot_nn(left[: 2 * UNITS], rows).astype(BF16)
        out_ref[b, 2 * UNITS : 3 * UNITS] = dot_nn(left[2 * UNITS :], errs).astype(BF16)
        here = jnp.where(w == 0, gains[:, 2 * b * 128 : (2 * b + 1) * 128], gains[:, (2 * b + 1) * 128 : (2 * b + 2) * 128])
        out_ref[b, 3 * UNITS :] = jnp.broadcast_to(here, (16, 128)).astype(BF16)


def totals(which, args):
    return pl.pallas_call(
        totals_body,
        out_shape=jax.ShapeDtypeStruct((8, ROWS, 128), BF16),
        in_specs=[pl.BlockSpec(memory_space=pltpu.SMEM)] + [pl.BlockSpec(memory_space=pltpu.VMEM)] * len(args),
        out_specs=pl.BlockSpec(memory_space=pltpu.VMEM),
        scratch_shapes=[pltpu.VMEM((3 * UNITS, STEPS * TOK), BF16)],
        compiler_params=pltpu.CompilerParams(vmem_limit_bytes=24 * 1024 * 1024),
    )(which, *args)


def pair_body(x, own, came, *outs):
    for h in range(2):
        for d in range(4):
            i = h * 4 + (x[0] + d) % 4
            outs[d][h] = (own[i].astype(F32) + came[i].astype(F32)).astype(BF16)


def line_body(hi, keep, one, two, three, near_ref, far_ref):
    def total(h):
        return keep[h].astype(F32) + one[h].astype(F32) + two[h].astype(F32) + three[h].astype(F32)

    near_ref[...] = total(hi[0])
    far_ref[...] = total(1 - hi[0]).astype(BF16)


def last_body(near, came, gate_ref, up_ref, down_ref, gain_ref):
    total = (near[...] + came[...].astype(F32)) * (1.0 / 16.0)
    gate_ref[...] = total[:UNITS].T
    up_ref[...] = total[UNITS : 2 * UNITS].T
    down_ref[...] = total[2 * UNITS : 3 * UNITS]
    gain_ref[...] = total[3 * UNITS : 3 * UNITS + 8]


def client_perm(dh, dx, dc):
    return [
        (h * 8 + x * 2 + c, ((h + dh) % 2) * 8 + ((x + dx) % 4) * 2 + (c + dc) % 2)
        for h in range(2)
        for x in range(4)
        for c in range(2)
    ]


def to_all(array, axis):
    return lax.all_to_all(array, axis, 0, 0, tiled=True)


def on_device(inputs, targets, norm_gain, gate_weight, up_weight, down_weight, overflow):
    x = inputs[0]
    first_row = lax.axis_index("tp") * 8
    own_x = lax.dynamic_slice_in_dim(x, first_row, 8, 0)
    own_t = lax.dynamic_slice_in_dim(targets[0], first_row, 8, 0)
    flags = overflow.reshape(STEPS)
    gain = norm_gain.reshape(1, D)
    gain_total = jnp.zeros((1, D), F32)
    weights = (gate_weight, up_weight, down_weight)
    row = ((1, D), F32)
    made = [((TOK, D), BF16), ((TOK, 2 * UNITS), F32), ((TOK, UNITS), BF16), ((16, 8, D), BF16)]
    past, factors, arrived = [], [], None
    for step in range(STEPS):
        flat = [r for p in past for r in p]
        if step == 0:
            scaled, normed, act, hidden, share = call(first_body, [((TOK, D), F32)] + made, (x, gain) + weights)
        else:
            body = lambda *refs, step=step: next_body(step, *refs)
            factor, gain, gain_total, normed, act, hidden, share = call(
                body, [((8, 128), F32), row, row] + made, (arrived, gain, gain_total, scaled) + weights + tuple(flat + factors)
            )
            factors = factors + [factor]
        (copies,) = call(error_body, [((16, 8, D), BF16)], (to_all(share, "tp"), own_x, own_t))
        error = to_all(copies, "tp")
        body = lambda *refs, step=step: back_body(step, *refs)
        grads, pay = call(
            body,
            [((TOK, 2 * UNITS), BF16), ((16, 8, 384), BF16)],
            (error,) + weights + (scaled, normed, act, hidden) + tuple(flat + factors),
            (flags,),
        )
        arrived = to_all(pay, "tp")
        past = past + [(normed, grads, hidden, error.reshape(TOK, D))]

    me = lax.axis_index("client")
    core, along, hi = me % 2, (me // 2) % 4, me // 8
    flat = [r for p in past for r in p]
    args = (arrived, gain_total, *flat, *factors)
    other = totals((1 - core).reshape(1), args)
    came = lax.ppermute(other, "client", client_perm(0, 0, 1))
    own = totals(core.reshape(1), args)
    half = ((2, ROWS, 128), BF16)
    keep, one, two, three = call(pair_body, [half] * 4, (own, came), (along.reshape(1),))
    moved = [lax.ppermute(a, "client", client_perm(0, d, 0)) for d, a in ((1, one), (2, two), (3, three))]
    near, far = call(
        line_body, [((ROWS, 128), F32), ((ROWS, 128), BF16)], (keep, *moved), (hi.reshape(1),)
    )
    came = lax.ppermute(far, "client", client_perm(1, 0, 0))
    gate, up, down, gains = call(
        last_body,
        [((128, UNITS), F32), ((128, UNITS), F32), ((UNITS, 128), F32), ((8, 128), F32)],
        (near, came),
    )
    return gate, up, down, gains[0]


def solution(mesh):
    placed = (
        P("client", None, None),
        P("client", None, None),
        P(),
        P(None, "tp"),
        P(None, "tp"),
        P("tp", None),
        P("client", None, "tp"),
    )
    return jax.shard_map(
        on_device,
        mesh=mesh,
        in_specs=placed,
        out_specs=(P("client", "tp"), P("client", "tp"), P("tp", "client"), P("client")),
        check_vma=False,
    )
```

```python
import math

import jax
import jax.numpy as jnp
from jax import lax
from jax.experimental import pallas as pl
from jax.experimental.pallas import tpu as pltpu
from jax.sharding import PartitionSpec as P

D = 2048
FF = 4096
STEPS = 3
RATE = 0.005
LIMIT = 0.5 * math.sqrt(3.0 * D * FF)
TOK = 128
UNITS = 256
LIMIT_BYTES = 20 * 1024 * 1024
ROWS = 3 * UNITS + 16


BF16 = jnp.bfloat16
F32 = jnp.float32


def dot_nn(a, b):
    return jnp.dot(a, b, preferred_element_type=F32)


def dot_nt(a, b):
    return lax.dot_general(a, b, (((1,), (1,)), ((), ())), preferred_element_type=F32)


def call(body, outs, args, scalars=()):
    return pl.pallas_call(
        body,
        out_shape=tuple(jax.ShapeDtypeStruct(s, d) for s, d in outs),
        in_specs=[pl.BlockSpec(memory_space=pltpu.SMEM)] * len(scalars)
        + [pl.BlockSpec(memory_space=pltpu.VMEM)] * len(args),
        out_specs=tuple(pl.BlockSpec(memory_space=pltpu.VMEM) for _ in outs),
        compiler_params=pltpu.CompilerParams(vmem_limit_bytes=LIMIT_BYTES),
    )(*scalars, *args)


def forward(normed, wg, wu, down, past, coefs, act_ref, hid_ref, part_ref):
    gate = dot_nn(normed, wg[...])
    up = dot_nn(normed, wu[...])
    for (n, g, h, e), a in zip(past, coefs):
        k = (dot_nt(normed, n[...]) * a).astype(BF16)
        gate = gate - dot_nn(k, g[:, :UNITS])
        up = up - dot_nn(k, g[:, UNITS:])
    act_ref[:, :UNITS] = gate
    act_ref[:, UNITS:] = up
    hidden = (gate * jax.nn.sigmoid(gate) * up).astype(BF16)
    hid_ref[...] = hidden
    share = dot_nn(hidden, down[...])
    for (n, g, h, e), a in zip(past, coefs):
        k = (dot_nt(hidden, h[...]) * a).astype(BF16)
        share = share - dot_nn(k, e[...])
    part_ref[...] = share.astype(BF16).reshape(16, 8, D)


def first_body(mine, me, x, t, gain, wg, wu, down, *refs):
    wg_ref, wu_ref, down_ref, diff_ref, scaled_ref, norm_ref, act_ref, hid_ref, part_ref = refs[:9]
    x_buf, x_own, t_own, sems = refs[9:]
    rows = pl.ds(pl.multiple_of(mine[0] * 8, 8), 8)
    moves = [(x, x_buf), (wg, wg_ref), (wu, wu_ref), (down, down_ref), (x.at[rows], x_own), (t.at[rows], t_own)]
    moves = [pltpu.make_async_copy(a, b, sems.at[i]) for i, (a, b) in enumerate(moves)]
    for m in moves:
        m.start()
    moves[0].wait()
    activ = x_buf[...].astype(F32)
    scaled = activ * lax.rsqrt(jnp.mean(activ * activ, axis=-1, keepdims=True) + 1e-05)
    scaled_ref[...] = scaled
    normed = (scaled * gain[...]).astype(BF16)
    norm_ref[...] = normed
    for m in moves[1:]:
        m.wait()
    diff_ref[...] = x_own[...].astype(F32) - t_own[...].astype(F32)
    forward(normed, wg_ref, wu_ref, down_ref, (), (), act_ref, hid_ref, part_ref)


def first(mine, me, x, t, gain, weights, outs):
    vmem, smem = pl.BlockSpec(memory_space=pltpu.VMEM), pl.BlockSpec(memory_space=pltpu.SMEM)
    far = pl.BlockSpec(memory_space=pltpu.HBM)
    return pl.pallas_call(
        first_body,
        out_shape=tuple(jax.ShapeDtypeStruct(s, d) for s, d in outs),
        in_specs=[smem, smem, far, far, vmem, far, far, far],
        out_specs=tuple(vmem for _ in outs),
        scratch_shapes=[
            pltpu.VMEM((TOK, D), BF16),
            pltpu.VMEM((8, D), BF16),
            pltpu.VMEM((8, D), BF16),
            pltpu.SemaphoreType.DMA((6,)),
        ],
        compiler_params=pltpu.CompilerParams(vmem_limit_bytes=47 * 1024 * 1024),
    )(mine, me, x, t, gain, *weights)


def sums_of(arrived):
    total = arrived[0].astype(F32)
    for i in range(1, 16):
        total = total + arrived[i].astype(F32)
    grad_gain = jnp.concatenate([total[r : r + 1, :256] for r in range(8)], axis=1)
    squares = jnp.sum(jnp.sum(total[0:3, 256:], axis=0, keepdims=True), axis=1, keepdims=True)
    squares = squares + jnp.sum(grad_gain * grad_gain, axis=1, keepdims=True)
    flagged = total[3:4, 256:257]
    norm = jnp.sqrt(squares + 1e-06)
    factor = jnp.where(flagged < 0.5, LIMIT / jnp.maximum(norm, LIMIT), 0.0)
    return grad_gain, factor


def next_body(step, *refs):
    arrived, gain, gain_total, scaled, wg, wu, down = refs[:7]
    at = 7
    past = [refs[at + 4 * j : at + 4 * j + 4] for j in range(step)]
    at += 4 * step
    old = refs[at : at + step - 1]
    at += step - 1
    factor_ref, gain_ref, total_ref, norm_ref, act_ref, hid_ref, part_ref = refs[at:]
    grad_gain, factor = sums_of(arrived)
    factor_ref[...] = jnp.broadcast_to(factor, (8, 128))
    new_gain = gain[...] - RATE * factor * grad_gain
    gain_ref[...] = new_gain
    total_ref[...] = gain_total[...] + factor * grad_gain
    normed = (scaled[...] * new_gain).astype(BF16)
    norm_ref[...] = normed
    coefs = [RATE * r[0:1, 0:1] for r in old] + [RATE * factor]
    forward(normed, wg, wu, down, past, coefs, act_ref, hid_ref, part_ref)


def error_body(arrived, diff, out_ref):
    total = arrived[0].astype(F32)
    for i in range(1, 16):
        total = total + arrived[i].astype(F32)
    error = (total + diff[...]).astype(BF16)
    for i in range(16):
        out_ref[i] = error


def pieces(value):
    first = value.astype(BF16)
    rest = value - first.astype(F32)
    second = rest.astype(BF16)
    third = (rest - second.astype(F32)).astype(BF16)
    return [first.astype(F32), second.astype(F32), third.astype(F32)]


def back_body(step, flags, *refs):
    error, wg, wu, down, scaled, normed, act, hidden = refs[:8]
    at = 8
    past = [refs[at + 4 * j : at + 4 * j + 4] for j in range(step)]
    at += 4 * step
    coefs = [RATE * r[0:1, 0:1] for r in refs[at : at + step]]
    at += step
    grad_ref, pay_ref = refs[at:]
    err = error[...].reshape(TOK, D)
    hid = hidden[...]
    nrm = normed[...]
    grad_hidden = dot_nt(err, down[...])
    for (n, g, h, e), a in zip(past, coefs):
        k = (dot_nt(err, e[...]) * a).astype(BF16)
        grad_hidden = grad_hidden - dot_nn(k, h[...])
    gate, up = act[:, :UNITS], act[:, UNITS:]
    sig = jax.nn.sigmoid(gate)
    g_gate = (grad_hidden * up * (sig * (1.0 + gate * (1.0 - sig)))).astype(BF16)
    g_up = (grad_hidden * (gate * sig)).astype(BF16)
    grad_ref[:, :UNITS] = g_gate
    grad_ref[:, UNITS:] = g_up
    grads = jnp.concatenate([g_gate, g_up], axis=1)
    grad_normed = dot_nt(g_gate, wg[...]) + dot_nt(g_up, wu[...])
    for (n, g, h, e), a in zip(past, coefs):
        k = (dot_nt(grads, g[...]) * a).astype(BF16)
        grad_normed = grad_normed - dot_nn(k, n[...])
    gain_part = jnp.sum(grad_normed * scaled[...], axis=0, keepdims=True)
    square = dot_nt(nrm, nrm) * dot_nt(grads, grads) + dot_nt(err, err) * dot_nt(hid, hid)
    square = jnp.sum(square, axis=0, keepdims=True)
    flag = jnp.full((1, 128), flags[step].astype(F32))
    tail = jnp.concatenate(pieces(square) + [flag, jnp.zeros((4, 128), F32)], axis=0)
    head = jnp.concatenate([gain_part[:, r * 256 : (r + 1) * 256] for r in range(8)], axis=0)
    packed = jnp.concatenate([head, tail], axis=1).astype(BF16)
    for i in range(16):
        pay_ref[i] = packed


def totals_body(flip, me, *refs):
    arrived, gain_total = refs[:2]
    past = [refs[2 + 4 * j : 6 + 4 * j] for j in range(STEPS)]
    old = refs[2 + 4 * STEPS : 2 + 4 * STEPS + STEPS - 1]
    out_ref, left = refs[2 + 4 * STEPS + STEPS - 1 :]
    grad_gain, factor = sums_of(arrived)
    gains = gain_total[...] + factor * grad_gain
    factors = [r[0:1, 0:1] for r in old] + [factor]
    for j, ((n, g, h, e), f) in enumerate(zip(past, factors)):
        left[: 2 * UNITS, j * TOK : (j + 1) * TOK] = (g[...].astype(F32) * f).T.astype(BF16)
        left[2 * UNITS :, j * TOK : (j + 1) * TOK] = (h[...].astype(F32) * f).T.astype(BF16)
    w = lax.rem(me[0] + flip, 2)
    for b in range(8):
        col = pl.ds(pl.multiple_of((2 * b + w) * 128, 128), 128)
        rows = jnp.concatenate([p[0][:, col] for p in past], axis=0)
        errs = jnp.concatenate([p[3][:, col] for p in past], axis=0)
        out_ref[b, : 2 * UNITS] = dot_nn(left[: 2 * UNITS], rows).astype(BF16)
        out_ref[b, 2 * UNITS : 3 * UNITS] = dot_nn(left[2 * UNITS :], errs).astype(BF16)
        here = jnp.where(w == 0, gains[:, 2 * b * 128 : (2 * b + 1) * 128], gains[:, (2 * b + 1) * 128 : (2 * b + 2) * 128])
        out_ref[b, 3 * UNITS :] = jnp.broadcast_to(here, (16, 128)).astype(BF16)


def totals(flip, me, args):
    return pl.pallas_call(
        lambda *refs: totals_body(flip, *refs),
        out_shape=jax.ShapeDtypeStruct((8, ROWS, 128), BF16),
        in_specs=[pl.BlockSpec(memory_space=pltpu.SMEM)] + [pl.BlockSpec(memory_space=pltpu.VMEM)] * len(args),
        out_specs=pl.BlockSpec(memory_space=pltpu.VMEM),
        scratch_shapes=[pltpu.VMEM((3 * UNITS, STEPS * TOK), BF16)],
        compiler_params=pltpu.CompilerParams(vmem_limit_bytes=LIMIT_BYTES),
    )(me, *args)


def pair_body(own, came, out_ref):
    for i in range(8):
        out_ref[i] = (own[i].astype(F32) + came[i].astype(F32)).astype(BF16)


def last_body(came, gate_ref, up_ref, down_ref, gain_ref):
    total = came[0].astype(F32)
    for i in range(1, 8):
        total = total + came[i].astype(F32)
    total = total * (1.0 / 16.0)
    gate_ref[...] = total[:UNITS].T
    up_ref[...] = total[UNITS : 2 * UNITS].T
    down_ref[...] = total[2 * UNITS : 3 * UNITS]
    gain_ref[...] = total[3 * UNITS : 3 * UNITS + 1]


def client_perm(dh, dx, dc):
    return [
        (h * 8 + x * 2 + c, ((h + dh) % 2) * 8 + ((x + dx) % 4) * 2 + (c + dc) % 2)
        for h in range(2)
        for x in range(4)
        for c in range(2)
    ]


def to_all(array, axis):
    return lax.all_to_all(array, axis, 0, 0, tiled=True)


def on_device(inputs, targets, norm_gain, gate_weight, up_weight, down_weight, overflow):
    mine = lax.axis_index("tp").reshape(1)
    me = lax.axis_index("client").reshape(1)
    flags = overflow.reshape(STEPS)
    gain = norm_gain.reshape(1, D)
    gain_total = jnp.zeros((1, D), F32)
    weights = (gate_weight, up_weight, down_weight)
    row = ((1, D), F32)
    made = [((TOK, D), BF16), ((TOK, 2 * UNITS), F32), ((TOK, UNITS), BF16), ((16, 8, D), BF16)]
    past, factors, arrived = [], [], None
    for step in range(STEPS):
        flat = [r for p in past for r in p]
        if step == 0:
            held = [((D, UNITS), BF16), ((D, UNITS), BF16), ((UNITS, D), BF16), ((8, D), F32), ((TOK, D), F32)]
            out = first(mine, me, inputs[0], targets[0], gain, weights, held + made)
            weights, (diff, scaled, normed, act, hidden, share) = out[:3], out[3:]
        else:
            body = lambda *refs, step=step: next_body(step, *refs)
            factor, gain, gain_total, normed, act, hidden, share = call(
                body, [((8, 128), F32), row, row] + made, (arrived, gain, gain_total, scaled) + weights + tuple(flat + factors)
            )
            factors = factors + [factor]
        (copies,) = call(error_body, [((16, 8, D), BF16)], (to_all(share, "tp"), diff))
        error = to_all(copies, "tp")
        body = lambda *refs, step=step: back_body(step, *refs)
        grads, pay = call(
            body,
            [((TOK, 2 * UNITS), BF16), ((16, 8, 384), BF16)],
            (error,) + weights + (scaled, normed, act, hidden) + tuple(flat + factors),
            (flags,),
        )
        arrived = to_all(pay, "tp")
        past = past + [(normed, grads, hidden, error.reshape(TOK, D))]

    flat = [r for p in past for r in p]
    args = (arrived, gain_total, *flat, *factors)
    other = totals(1, me, args)
    came = lax.ppermute(other, "client", client_perm(0, 0, 1))
    own = totals(0, me, args)
    (pair,) = call(pair_body, [((8, ROWS, 128), BF16)], (own, came))
    groups = [[2 * i + c for i in range(8)] for c in range(2)]
    came = lax.all_to_all(pair, "client", 0, 0, tiled=True, axis_index_groups=groups)
    gate, up, down, gains = call(
        last_body,
        [((128, UNITS), F32), ((128, UNITS), F32), ((UNITS, 128), F32), ((1, 128), F32)],
        (came,),
    )
    return gate, up, down, gains.reshape(128)


def solution(mesh):
    placed = (
        P("client", None, None),
        P("client", None, None),
        P(),
        P(None, "tp"),
        P(None, "tp"),
        P("tp", None),
        P("client", None, "tp"),
    )
    return jax.shard_map(
        on_device,
        mesh=mesh,
        in_specs=placed,
        out_specs=(P("client", "tp"), P("client", "tp"), P("tp", "client"), P("client")),
        check_vma=False,
    )
```

```python
import math

import jax
import jax.numpy as jnp
from jax import lax
from jax.experimental import pallas as pl
from jax.experimental.pallas import tpu as pltpu
from jax.sharding import PartitionSpec as P

D = 2048
FF = 4096
STEPS = 3
RATE = 0.005
LIMIT = 0.5 * math.sqrt(3.0 * D * FF)
TOK = 128
UNITS = 256
BLOCK = 32
LIMIT_BYTES = 20 * 1024 * 1024
FIRST_BYTES = 48 * 1024 * 1024
ROWS = 3 * UNITS + 16


BF16 = jnp.bfloat16
F32 = jnp.float32


def dot_nn(a, b):
    return jnp.dot(a, b, preferred_element_type=F32)


def dot_nt(a, b):
    return lax.dot_general(a, b, (((1,), (1,)), ((), ())), preferred_element_type=F32)


def call(body, outs, args, scalars=()):
    return pl.pallas_call(
        body,
        out_shape=tuple(jax.ShapeDtypeStruct(s, d) for s, d in outs),
        in_specs=[pl.BlockSpec(memory_space=pltpu.SMEM)] * len(scalars)
        + [pl.BlockSpec(memory_space=pltpu.VMEM)] * len(args),
        out_specs=tuple(pl.BlockSpec(memory_space=pltpu.VMEM) for _ in outs),
        compiler_params=pltpu.CompilerParams(vmem_limit_bytes=LIMIT_BYTES),
    )(*scalars, *args)


def token_block(i):
    return pl.ds(pl.multiple_of(lax.rem(i, 4) * BLOCK, BLOCK), BLOCK)


def forward(y, normed, wg, wu, down, past, coefs, act_ref, hid_ref, *part_refs):
    gate = dot_nn(normed, wg[...])
    up = dot_nn(normed, wu[...])
    for (n, g, h, e), a in zip(past, coefs):
        k = (dot_nt(normed, n[...]) * a).astype(BF16)
        gate = gate - dot_nn(k, g[:, :UNITS])
        up = up - dot_nn(k, g[:, UNITS:])
    act_ref[:, :UNITS] = gate
    act_ref[:, UNITS:] = up
    hidden = (gate * jax.nn.sigmoid(gate) * up).astype(BF16)
    hid_ref[...] = hidden
    turned = jnp.concatenate([hid_ref[token_block(y + d)] for d in range(4)], axis=0)
    share = dot_nn(turned, down[...])
    for (n, g, h, e), a in zip(past, coefs):
        k = (dot_nt(turned, h[...]) * a).astype(BF16)
        share = share - dot_nn(k, e[...])
    for d in range(4):
        part_refs[d][...] = share[d * BLOCK : (d + 1) * BLOCK].astype(BF16)


def first_body(mine, me, x, gain, wg, wu, down, *refs):
    wg_ref, wu_ref, down_ref, scaled_ref, norm_ref, act_ref, hid_ref = refs[:7]
    part_refs = refs[7:11]
    x_buf, sems = refs[11:]
    moves = [(x, x_buf), (wg, wg_ref), (wu, wu_ref), (down, down_ref)]
    moves = [pltpu.make_async_copy(a, b, sems.at[i]) for i, (a, b) in enumerate(moves)]
    for m in moves:
        m.start()
    moves[0].wait()
    activ = x_buf[...].astype(F32)
    scaled = activ * lax.rsqrt(jnp.mean(activ * activ, axis=-1, keepdims=True) + 1e-05)
    scaled_ref[...] = scaled
    normed = (scaled * gain[...]).astype(BF16)
    norm_ref[...] = normed
    for m in moves[1:]:
        m.wait()
    forward(mine[0] // 4, normed, wg_ref, wu_ref, down_ref, (), (), act_ref, hid_ref, *part_refs)


def first(mine, me, x, gain, weights, outs):
    vmem, smem = pl.BlockSpec(memory_space=pltpu.VMEM), pl.BlockSpec(memory_space=pltpu.SMEM)
    far = pl.BlockSpec(memory_space=pltpu.HBM)
    return pl.pallas_call(
        first_body,
        out_shape=tuple(jax.ShapeDtypeStruct(s, d) for s, d in outs),
        in_specs=[smem, smem, far, vmem, far, far, far],
        out_specs=tuple(vmem for _ in outs),
        scratch_shapes=[pltpu.VMEM((TOK, D), BF16), pltpu.SemaphoreType.DMA((4,))],
        compiler_params=pltpu.CompilerParams(vmem_limit_bytes=FIRST_BYTES),
    )(mine, me, x, gain, *weights)


def sums_of(arrived):
    total = arrived[0].astype(F32)
    for i in range(1, 16):
        total = total + arrived[i].astype(F32)
    grad_gain = jnp.concatenate([total[r : r + 1, :256] for r in range(8)], axis=1)
    squares = jnp.sum(jnp.sum(total[0:3, 256:], axis=0, keepdims=True), axis=1, keepdims=True)
    squares = squares + jnp.sum(grad_gain * grad_gain, axis=1, keepdims=True)
    flagged = total[3:4, 256:257]
    norm = jnp.sqrt(squares + 1e-06)
    factor = jnp.where(flagged < 0.5, LIMIT / jnp.maximum(norm, LIMIT), 0.0)
    return grad_gain, factor


def next_body(step, mine, *refs):
    arrived, gain, gain_total, scaled, wg, wu, down = refs[:7]
    at = 7
    past = [refs[at + 4 * j : at + 4 * j + 4] for j in range(step)]
    at += 4 * step
    old = refs[at : at + step - 1]
    at += step - 1
    factor_ref, gain_ref, total_ref, norm_ref, act_ref, hid_ref = refs[at : at + 6]
    part_refs = refs[at + 6 :]
    grad_gain, factor = sums_of(arrived)
    factor_ref[...] = jnp.broadcast_to(factor, (8, 128))
    new_gain = gain[...] - RATE * factor * grad_gain
    gain_ref[...] = new_gain
    total_ref[...] = gain_total[...] + factor * grad_gain
    normed = (scaled[...] * new_gain).astype(BF16)
    norm_ref[...] = normed
    coefs = [RATE * r[0:1, 0:1] for r in old] + [RATE * factor]
    forward(mine[0] // 4, normed, wg, wu, down, past, coefs, act_ref, hid_ref, *part_refs)


def summed(refs):
    total = refs[0][...].astype(F32)
    for r in refs[1:]:
        total = total + r[...].astype(F32)
    return total


def row_body(*refs):
    refs[-1][...] = summed(refs[:-1]).astype(BF16)


def first_error_body(mine, a, b, c, d, x, t, out_ref, diff_ref):
    rows = token_block(mine[0] // 4)
    diff = x[rows].astype(F32) - t[rows].astype(F32)
    diff_ref[...] = diff
    out_ref[...] = (summed((a, b, c, d)) + diff).astype(BF16)


def error_body(a, b, c, d, diff, out_ref):
    out_ref[...] = (summed((a, b, c, d)) + diff[...]).astype(BF16)


def pieces(value):
    first = value.astype(BF16)
    rest = value - first.astype(F32)
    second = rest.astype(BF16)
    third = (rest - second.astype(F32)).astype(BF16)
    return [first.astype(F32), second.astype(F32), third.astype(F32)]


def back_body(step, flags, mine, *refs):
    errors, (wg, wu, down, scaled, normed, act, hidden) = refs[:4], refs[4:11]
    at = 11
    past = [refs[at + 4 * j : at + 4 * j + 4] for j in range(step)]
    at += 4 * step
    coefs = [RATE * r[0:1, 0:1] for r in refs[at : at + step]]
    at += step
    err_ref, grad_ref, pay_ref = refs[at:]
    for d in range(4):
        err_ref[token_block(mine[0] // 4 + 4 - d)] = errors[d][...]
    err = err_ref[...]
    hid = hidden[...]
    nrm = normed[...]
    grad_hidden = dot_nt(err, down[...])
    for (n, g, h, e), a in zip(past, coefs):
        k = (dot_nt(err, e[...]) * a).astype(BF16)
        grad_hidden = grad_hidden - dot_nn(k, h[...])
    gate, up = act[:, :UNITS], act[:, UNITS:]
    sig = jax.nn.sigmoid(gate)
    g_gate = (grad_hidden * up * (sig * (1.0 + gate * (1.0 - sig)))).astype(BF16)
    g_up = (grad_hidden * (gate * sig)).astype(BF16)
    grad_ref[:, :UNITS] = g_gate
    grad_ref[:, UNITS:] = g_up
    grads = jnp.concatenate([g_gate, g_up], axis=1)
    grad_normed = dot_nt(g_gate, wg[...]) + dot_nt(g_up, wu[...])
    for (n, g, h, e), a in zip(past, coefs):
        k = (dot_nt(grads, g[...]) * a).astype(BF16)
        grad_normed = grad_normed - dot_nn(k, n[...])
    gain_part = jnp.sum(grad_normed * scaled[...], axis=0, keepdims=True)
    square = dot_nt(nrm, nrm) * dot_nt(grads, grads) + dot_nt(err, err) * dot_nt(hid, hid)
    square = jnp.sum(square, axis=0, keepdims=True)
    flag = jnp.full((1, 128), flags[step].astype(F32))
    tail = jnp.concatenate(pieces(square) + [flag, jnp.zeros((4, 128), F32)], axis=0)
    head = jnp.concatenate([gain_part[:, r * 256 : (r + 1) * 256] for r in range(8)], axis=0)
    packed = jnp.concatenate([head, tail], axis=1).astype(BF16)
    for i in range(16):
        pay_ref[i] = packed


def totals_body(flip, me, *refs):
    arrived, gain_total = refs[:2]
    past = [refs[2 + 4 * j : 6 + 4 * j] for j in range(STEPS)]
    old = refs[2 + 4 * STEPS : 2 + 4 * STEPS + STEPS - 1]
    out_ref, left = refs[2 + 4 * STEPS + STEPS - 1 :]
    grad_gain, factor = sums_of(arrived)
    gains = gain_total[...] + factor * grad_gain
    factors = [r[0:1, 0:1] for r in old] + [factor]
    for j, ((n, g, h, e), f) in enumerate(zip(past, factors)):
        left[: 2 * UNITS, j * TOK : (j + 1) * TOK] = (g[...].astype(F32) * f).T.astype(BF16)
        left[2 * UNITS :, j * TOK : (j + 1) * TOK] = (h[...].astype(F32) * f).T.astype(BF16)
    w = lax.rem(me[0] + flip, 2)
    for b in range(8):
        col = pl.ds(pl.multiple_of((2 * b + w) * 128, 128), 128)
        rows = jnp.concatenate([p[0][:, col] for p in past], axis=0)
        errs = jnp.concatenate([p[3][:, col] for p in past], axis=0)
        out_ref[b, : 2 * UNITS] = dot_nn(left[: 2 * UNITS], rows).astype(BF16)
        out_ref[b, 2 * UNITS : 3 * UNITS] = dot_nn(left[2 * UNITS :], errs).astype(BF16)
        here = jnp.where(w == 0, gains[:, 2 * b * 128 : (2 * b + 1) * 128], gains[:, (2 * b + 1) * 128 : (2 * b + 2) * 128])
        out_ref[b, 3 * UNITS :] = jnp.broadcast_to(here, (16, 128)).astype(BF16)


def totals(flip, me, args):
    return pl.pallas_call(
        lambda *refs: totals_body(flip, *refs),
        out_shape=jax.ShapeDtypeStruct((8, ROWS, 128), BF16),
        in_specs=[pl.BlockSpec(memory_space=pltpu.SMEM)] + [pl.BlockSpec(memory_space=pltpu.VMEM)] * len(args),
        out_specs=pl.BlockSpec(memory_space=pltpu.VMEM),
        scratch_shapes=[pltpu.VMEM((3 * UNITS, STEPS * TOK), BF16)],
        compiler_params=pltpu.CompilerParams(vmem_limit_bytes=LIMIT_BYTES),
    )(me, *args)


def pair_body(me, own, came, *outs):
    x = lax.rem(me[0] // 2, 4)
    for h in range(2):
        for d in range(4):
            i = h * 4 + lax.rem(x + d, 4)
            outs[d][h] = (own[i].astype(F32) + came[i].astype(F32)).astype(BF16)


def line_body(me, keep, one, two, three, near_ref, far_ref):
    def total(h):
        return keep[h].astype(F32) + one[h].astype(F32) + two[h].astype(F32) + three[h].astype(F32)

    h = me[0] // 8
    near_ref[...] = total(h)
    far_ref[...] = total(1 - h).astype(BF16)


def last_body(near, came, gate_ref, up_ref, down_ref, gain_ref):
    total = (near[...] + came[...].astype(F32)) * (1.0 / 16.0)
    gate_ref[...] = total[:UNITS].T
    up_ref[...] = total[UNITS : 2 * UNITS].T
    down_ref[...] = total[2 * UNITS : 3 * UNITS]
    gain_ref[...] = total[3 * UNITS : 3 * UNITS + 1]


def client_perm(dh, dx, dc):
    return [
        (h * 8 + x * 2 + c, ((h + dh) % 2) * 8 + ((x + dx) % 4) * 2 + (c + dc) % 2)
        for h in range(2)
        for x in range(4)
        for c in range(2)
    ]


def tp_perm(dy, dz):
    return [(y * 4 + z, (y + dy) % 4 * 4 + (z + dz) % 4) for y in range(4) for z in range(4)]


def along_y(array, d):
    return lax.ppermute(array, "tp", tp_perm(d, 0))


def along_z(array, d):
    return lax.ppermute(array, "tp", tp_perm(0, d))


def to_all(array, axis):
    return lax.all_to_all(array, axis, 0, 0, tiled=True)


def on_device(inputs, targets, norm_gain, gate_weight, up_weight, down_weight, overflow):
    mine = lax.axis_index("tp").reshape(1)
    me = lax.axis_index("client").reshape(1)
    flags = overflow.reshape(STEPS)
    gain = norm_gain.reshape(1, D)
    gain_total = jnp.zeros((1, D), F32)
    weights = (gate_weight, up_weight, down_weight)
    row = ((1, D), F32)
    made = [((TOK, D), BF16), ((TOK, 2 * UNITS), F32), ((TOK, UNITS), BF16)] + [((BLOCK, D), BF16)] * 4
    past, factors, arrived, diff = [], [], None, None
    for step in range(STEPS):
        flat = [r for p in past for r in p]
        if step == 0:
            held = [((D, UNITS), BF16), ((D, UNITS), BF16), ((UNITS, D), BF16), ((TOK, D), F32)]
            out = first(mine, me, inputs[0], gain, weights, held + made)
            weights, (scaled, normed, act, hidden, *parts) = out[:3], out[3:]
        else:
            body = lambda *refs, step=step: next_body(step, *refs)
            factor, gain, gain_total, normed, act, hidden, *parts = call(
                body,
                [((8, 128), F32), row, row] + made,
                (arrived, gain, gain_total, scaled) + weights + tuple(flat + factors),
                (mine,),
            )
            factors = factors + [factor]
        block = ((BLOCK, D), BF16)
        (rows,) = call(row_body, [block], (parts[0], *[along_y(parts[d], d) for d in (1, 2, 3)]))
        came = [along_z(rows, d) for d in (1, 2, 3)]
        if step == 0:
            error, diff = call(first_error_body, [block, ((BLOCK, D), F32)], (rows, *came, inputs[0], targets[0]), (mine,))
        else:
            (error,) = call(error_body, [block], (rows, *came, diff))
        errors = (error, *[along_y(error, d) for d in (1, 2, 3)])
        body = lambda *refs, step=step: back_body(step, *refs)
        error, grads, pay = call(
            body,
            [((TOK, D), BF16), ((TOK, 2 * UNITS), BF16), ((16, 8, 384), BF16)],
            errors + weights + (scaled, normed, act, hidden) + tuple(flat + factors),
            (flags, mine),
        )
        arrived = to_all(pay, "tp")
        past = past + [(normed, grads, hidden, error)]

    flat = [r for p in past for r in p]
    args = (arrived, gain_total, *flat, *factors)
    other = totals(1, me, args)
    came = lax.ppermute(other, "client", client_perm(0, 0, 1))
    own = totals(0, me, args)
    half = ((2, ROWS, 128), BF16)
    keep, one, two, three = call(pair_body, [half] * 4, (own, came), (me,))
    moved = [lax.ppermute(a, "client", client_perm(0, d, 0)) for d, a in ((1, one), (2, two), (3, three))]
    near, far = call(line_body, [((ROWS, 128), F32), ((ROWS, 128), BF16)], (keep, *moved), (me,))
    came = lax.ppermute(far, "client", client_perm(1, 0, 0))
    gate, up, down, gains = call(
        last_body,
        [((128, UNITS), F32), ((128, UNITS), F32), ((UNITS, 128), F32), ((1, 128), F32)],
        (near, came),
    )
    return gate, up, down, gains.reshape(128)


def solution(mesh):
    placed = (
        P("client", None, None),
        P("client", None, None),
        P(),
        P(None, "tp"),
        P(None, "tp"),
        P("tp", None),
        P("client", None, "tp"),
    )
    return jax.shard_map(
        on_device,
        mesh=mesh,
        in_specs=placed,
        out_specs=(P("client", "tp"), P("client", "tp"), P("tp", "client"), P("client")),
        check_vma=False,
    )
```

```python
import math

import jax
import jax.numpy as jnp
from jax import lax
from jax.experimental import pallas as pl
from jax.experimental.pallas import tpu as pltpu
from jax.sharding import PartitionSpec as P

D = 2048
FF = 4096
STEPS = 3
RATE = 0.005
LIMIT = 0.5 * math.sqrt(3.0 * D * FF)
TOK = 128
UNITS = 256
BLOCK = 32
LIMIT_BYTES = 20 * 1024 * 1024
FIRST_BYTES = 50 * 1024 * 1024
ROWS = 3 * UNITS + 16
CUT = 400


BF16 = jnp.bfloat16
F32 = jnp.float32


def dot_nn(a, b):
    return jnp.dot(a, b, preferred_element_type=F32)


def dot_nt(a, b):
    return lax.dot_general(a, b, (((1,), (1,)), ((), ())), preferred_element_type=F32)


def call(body, outs, args, scalars=()):
    return pl.pallas_call(
        body,
        out_shape=tuple(jax.ShapeDtypeStruct(s, d) for s, d in outs),
        in_specs=[pl.BlockSpec(memory_space=pltpu.SMEM)] * len(scalars)
        + [pl.BlockSpec(memory_space=pltpu.VMEM)] * len(args),
        out_specs=tuple(pl.BlockSpec(memory_space=pltpu.VMEM) for _ in outs),
        compiler_params=pltpu.CompilerParams(vmem_limit_bytes=LIMIT_BYTES),
    )(*scalars, *args)


def token_block(i):
    return pl.ds(pl.multiple_of(lax.rem(i, 4) * BLOCK, BLOCK), BLOCK)


def forward(y, normed, wg, wu, down, past, coefs, act_ref, hid_ref, *part_refs):
    gate = dot_nn(normed, wg[...])
    up = dot_nn(normed, wu[...])
    for (n, g, h, e), a in zip(past, coefs):
        k = (dot_nt(normed, n[...]) * a).astype(BF16)
        gate = gate - dot_nn(k, g[:, :UNITS])
        up = up - dot_nn(k, g[:, UNITS:])
    act_ref[:, :UNITS] = gate
    act_ref[:, UNITS:] = up
    hidden = (gate * jax.nn.sigmoid(gate) * up).astype(BF16)
    hid_ref[...] = hidden
    turned = jnp.concatenate([hid_ref[token_block(y + d)] for d in range(4)], axis=0)
    share = dot_nn(turned, down[...])
    for (n, g, h, e), a in zip(past, coefs):
        k = (dot_nt(turned, h[...]) * a).astype(BF16)
        share = share - dot_nn(k, e[...])
    for d in range(4):
        part_refs[d][...] = share[d * BLOCK : (d + 1) * BLOCK].astype(BF16)


def weights_body(me, wg, wu, down, wg_ref, wu_ref, down_ref, sems):
    moves = [(wg, wg_ref), (wu, wu_ref), (down, down_ref)]
    moves = [pltpu.make_async_copy(a, b, sems.at[i]) for i, (a, b) in enumerate(moves)]
    for m in moves:
        m.start()
    for m in moves:
        m.wait()


def in_vmem(me, weights):
    vmem, far = pl.BlockSpec(memory_space=pltpu.VMEM), pl.BlockSpec(memory_space=pltpu.HBM)
    return pl.pallas_call(
        weights_body,
        out_shape=tuple(jax.ShapeDtypeStruct(w.shape, w.dtype) for w in weights),
        in_specs=[pl.BlockSpec(memory_space=pltpu.SMEM), far, far, far],
        out_specs=(vmem, vmem, vmem),
        scratch_shapes=[pltpu.SemaphoreType.DMA((3,))],
        compiler_params=pltpu.CompilerParams(vmem_limit_bytes=FIRST_BYTES),
    )(me, *weights)


def first_body(mine, x, gain, wg, wu, down, scaled_ref, norm_ref, act_ref, hid_ref, *part_refs):
    activ = x[...].astype(F32)
    scaled = activ * lax.rsqrt(jnp.mean(activ * activ, axis=-1, keepdims=True) + 1e-05)
    scaled_ref[...] = scaled
    normed = (scaled * gain[...]).astype(BF16)
    norm_ref[...] = normed
    forward(mine[0] // 4, normed, wg, wu, down, (), (), act_ref, hid_ref, *part_refs)


def sums_of(arrived):
    total = arrived[0].astype(F32)
    for i in range(1, 16):
        total = total + arrived[i].astype(F32)
    grad_gain = jnp.concatenate([total[r : r + 1, :256] for r in range(8)], axis=1)
    squares = jnp.sum(jnp.sum(total[0:3, 256:], axis=0, keepdims=True), axis=1, keepdims=True)
    squares = squares + jnp.sum(grad_gain * grad_gain, axis=1, keepdims=True)
    flagged = total[3:4, 256:257]
    norm = jnp.sqrt(squares + 1e-06)
    factor = jnp.where(flagged < 0.5, LIMIT / jnp.maximum(norm, LIMIT), 0.0)
    return grad_gain, factor


def next_body(step, mine, *refs):
    arrived, gain, gain_total, scaled, wg, wu, down = refs[:7]
    at = 7
    past = [refs[at + 4 * j : at + 4 * j + 4] for j in range(step)]
    at += 4 * step
    old = refs[at : at + step - 1]
    at += step - 1
    factor_ref, gain_ref, total_ref, norm_ref, act_ref, hid_ref = refs[at : at + 6]
    part_refs = refs[at + 6 :]
    grad_gain, factor = sums_of(arrived)
    factor_ref[...] = jnp.broadcast_to(factor, (8, 128))
    new_gain = gain[...] - RATE * factor * grad_gain
    gain_ref[...] = new_gain
    total_ref[...] = gain_total[...] + factor * grad_gain
    normed = (scaled[...] * new_gain).astype(BF16)
    norm_ref[...] = normed
    coefs = [RATE * r[0:1, 0:1] for r in old] + [RATE * factor]
    forward(mine[0] // 4, normed, wg, wu, down, past, coefs, act_ref, hid_ref, *part_refs)


def summed(refs):
    total = refs[0][...].astype(F32)
    for r in refs[1:]:
        total = total + r[...].astype(F32)
    return total


def row_body(*refs):
    refs[-1][...] = summed(refs[:-1]).astype(BF16)


def first_error_body(mine, a, b, c, d, x, t, out_ref, diff_ref):
    rows = token_block(mine[0] // 4)
    diff = x[rows].astype(F32) - t[rows].astype(F32)
    diff_ref[...] = diff
    out_ref[...] = (summed((a, b, c, d)) + diff).astype(BF16)


def error_body(a, b, c, d, diff, out_ref):
    out_ref[...] = (summed((a, b, c, d)) + diff[...]).astype(BF16)


def pieces(value):
    first = value.astype(BF16)
    rest = value - first.astype(F32)
    second = rest.astype(BF16)
    third = (rest - second.astype(F32)).astype(BF16)
    return [first.astype(F32), second.astype(F32), third.astype(F32)]


def back_body(step, flags, mine, *refs):
    errors, (wg, wu, down, scaled, normed, act, hidden) = refs[:4], refs[4:11]
    at = 11
    past = [refs[at + 4 * j : at + 4 * j + 4] for j in range(step)]
    at += 4 * step
    coefs = [RATE * r[0:1, 0:1] for r in refs[at : at + step]]
    at += step
    err_ref, grad_ref, pay_ref = refs[at:]
    for d in range(4):
        err_ref[token_block(mine[0] // 4 + 4 - d)] = errors[d][...]
    err = err_ref[...]
    hid = hidden[...]
    nrm = normed[...]
    grad_hidden = dot_nt(err, down[...])
    for (n, g, h, e), a in zip(past, coefs):
        k = (dot_nt(err, e[...]) * a).astype(BF16)
        grad_hidden = grad_hidden - dot_nn(k, h[...])
    gate, up = act[:, :UNITS], act[:, UNITS:]
    sig = jax.nn.sigmoid(gate)
    g_gate = (grad_hidden * up * (sig * (1.0 + gate * (1.0 - sig)))).astype(BF16)
    g_up = (grad_hidden * (gate * sig)).astype(BF16)
    grad_ref[:, :UNITS] = g_gate
    grad_ref[:, UNITS:] = g_up
    grads = jnp.concatenate([g_gate, g_up], axis=1)
    grad_normed = dot_nt(g_gate, wg[...]) + dot_nt(g_up, wu[...])
    for (n, g, h, e), a in zip(past, coefs):
        k = (dot_nt(grads, g[...]) * a).astype(BF16)
        grad_normed = grad_normed - dot_nn(k, n[...])
    gain_part = jnp.sum(grad_normed * scaled[...], axis=0, keepdims=True)
    square = dot_nt(nrm, nrm) * dot_nt(grads, grads) + dot_nt(err, err) * dot_nt(hid, hid)
    square = jnp.sum(square, axis=0, keepdims=True)
    flag = jnp.full((1, 128), flags[step].astype(F32))
    tail = jnp.concatenate(pieces(square) + [flag, jnp.zeros((4, 128), F32)], axis=0)
    head = jnp.concatenate([gain_part[:, r * 256 : (r + 1) * 256] for r in range(8)], axis=0)
    packed = jnp.concatenate([head, tail], axis=1).astype(BF16)
    for i in range(16):
        pay_ref[i] = packed


def totals_body(flip, me, *refs):
    arrived, gain_total = refs[:2]
    past = [refs[2 + 4 * j : 6 + 4 * j] for j in range(STEPS)]
    old = refs[2 + 4 * STEPS : 2 + 4 * STEPS + STEPS - 1]
    out_ref, left, gain_row = refs[2 + 4 * STEPS + STEPS - 1 :]
    grad_gain, factor = sums_of(arrived)
    gains = gain_total[...] + factor * grad_gain
    factors = [r[0:1, 0:1] for r in old] + [factor]
    for j, ((n, g, h, e), f) in enumerate(zip(past, factors)):
        left[: 2 * UNITS, j * TOK : (j + 1) * TOK] = (g[...].astype(F32) * f).T.astype(BF16)
        left[2 * UNITS :, j * TOK : (j + 1) * TOK] = (h[...].astype(F32) * f).T.astype(BF16)
    gain_row[...] = gains
    w = lax.rem(me[0] + flip, 2)

    def two_blocks(i, carry):
        for b in (2 * i, 2 * i + 1):
            col = pl.ds(pl.multiple_of((2 * b + w) * 128, 128), 128)
            rows = jnp.concatenate([p[0][:, col] for p in past], axis=0)
            errs = jnp.concatenate([p[3][:, col] for p in past], axis=0)
            out_ref[b, : 2 * UNITS] = dot_nn(left[: 2 * UNITS], rows).astype(BF16)
            out_ref[b, 2 * UNITS : 3 * UNITS] = dot_nn(left[2 * UNITS :], errs).astype(BF16)
            out_ref[b, 3 * UNITS :] = jnp.broadcast_to(gain_row[:, col], (16, 128)).astype(BF16)
        return carry

    lax.fori_loop(0, 4, two_blocks, 0)


def totals(flip, me, args):
    return pl.pallas_call(
        lambda *refs: totals_body(flip, *refs),
        out_shape=jax.ShapeDtypeStruct((8, ROWS, 128), BF16),
        in_specs=[pl.BlockSpec(memory_space=pltpu.SMEM)] + [pl.BlockSpec(memory_space=pltpu.VMEM)] * len(args),
        out_specs=pl.BlockSpec(memory_space=pltpu.VMEM),
        scratch_shapes=[pltpu.VMEM((3 * UNITS, STEPS * TOK), BF16), pltpu.VMEM((1, D), F32)],
        compiler_params=pltpu.CompilerParams(vmem_limit_bytes=LIMIT_BYTES),
    )(me, *args)


def pair_body(me, own, came, *outs):
    x, h = lax.rem(me[0] // 2, 4), me[0] // 8
    for g in range(2):
        for d in range(4):
            i = g * 4 + lax.rem(x + d, 4)
            outs[d][g] = (own[i, :CUT].astype(F32) + came[i, :CUT].astype(F32)).astype(BF16)
    for d in range(2):
        for k in range(4):
            i = lax.rem(h + d, 2) * 4 + k
            outs[4 + d][k] = (own[i, CUT:].astype(F32) + came[i, CUT:].astype(F32)).astype(BF16)


def cross_body(me, keep, one, two, three, near, far, stay_ref, go_ref, *outs):
    x, h = lax.rem(me[0] // 2, 4), me[0] // 8

    def total(g):
        return keep[g].astype(F32) + one[g].astype(F32) + two[g].astype(F32) + three[g].astype(F32)

    stay_ref[...] = total(h)
    go_ref[...] = total(1 - h).astype(BF16)
    for d in range(4):
        i = lax.rem(x + d, 4)
        outs[d][...] = (near[i].astype(F32) + far[i].astype(F32)).astype(BF16)


def last_body(stay, came, a, b, c, d, gate_ref, up_ref, down_ref, gain_ref):
    top = (stay[...] + came[...].astype(F32)) * (1.0 / 16.0)
    total = jnp.concatenate([top, summed((a, b, c, d)) * (1.0 / 16.0)], axis=0)
    gate_ref[...] = total[:UNITS].T
    up_ref[...] = total[UNITS : 2 * UNITS].T
    down_ref[...] = total[2 * UNITS : 3 * UNITS]
    gain_ref[...] = total[3 * UNITS : 3 * UNITS + 1]


def client_perm(dh, dx, dc):
    return [
        (h * 8 + x * 2 + c, ((h + dh) % 2) * 8 + ((x + dx) % 4) * 2 + (c + dc) % 2)
        for h in range(2)
        for x in range(4)
        for c in range(2)
    ]


def along_client(array, dh, dx):
    return lax.ppermute(array, "client", client_perm(dh, dx, 0))


def tp_perm(dy, dz):
    return [(y * 4 + z, (y + dy) % 4 * 4 + (z + dz) % 4) for y in range(4) for z in range(4)]


def along_y(array, d):
    return lax.ppermute(array, "tp", tp_perm(d, 0))


def along_z(array, d):
    return lax.ppermute(array, "tp", tp_perm(0, d))


def to_all(array, axis):
    return lax.all_to_all(array, axis, 0, 0, tiled=True)


def on_device(inputs, targets, norm_gain, gate_weight, up_weight, down_weight, overflow):
    mine = lax.axis_index("tp").reshape(1)
    me = lax.axis_index("client").reshape(1)
    flags = overflow.reshape(STEPS)
    gain = norm_gain.reshape(1, D)
    gain_total = jnp.zeros((1, D), F32)
    weights = tuple(in_vmem(me, (gate_weight, up_weight, down_weight)))
    row = ((1, D), F32)
    made = [((TOK, D), BF16), ((TOK, 2 * UNITS), F32), ((TOK, UNITS), BF16)] + [((BLOCK, D), BF16)] * 4
    past, factors, arrived, diff = [], [], None, None
    for step in range(STEPS):
        flat = [r for p in past for r in p]
        if step == 0:
            scaled, normed, act, hidden, *parts = call(
                first_body, [((TOK, D), F32)] + made, (inputs[0], gain) + weights, (mine,)
            )
        else:
            body = lambda *refs, step=step: next_body(step, *refs)
            factor, gain, gain_total, normed, act, hidden, *parts = call(
                body,
                [((8, 128), F32), row, row] + made,
                (arrived, gain, gain_total, scaled) + weights + tuple(flat + factors),
                (mine,),
            )
            factors = factors + [factor]
        block = ((BLOCK, D), BF16)
        (rows,) = call(row_body, [block], (parts[0], *[along_y(parts[d], d) for d in (1, 2, 3)]))
        came = [along_z(rows, d) for d in (1, 2, 3)]
        if step == 0:
            error, diff = call(first_error_body, [block, ((BLOCK, D), F32)], (rows, *came, inputs[0], targets[0]), (mine,))
        else:
            (error,) = call(error_body, [block], (rows, *came, diff))
        errors = (error, *[along_y(error, d) for d in (1, 2, 3)])
        body = lambda *refs, step=step: back_body(step, *refs)
        error, grads, pay = call(
            body,
            [((TOK, D), BF16), ((TOK, 2 * UNITS), BF16), ((16, 8, 384), BF16)],
            errors + weights + (scaled, normed, act, hidden) + tuple(flat + factors),
            (flags, mine),
        )
        arrived = to_all(pay, "tp")
        past = past + [(normed, grads, hidden, error)]

    flat = [r for p in past for r in p]
    args = (arrived, gain_total, *flat, *factors)
    other = totals(1, me, args)
    came = lax.ppermute(other, "client", client_perm(0, 0, 1))
    own = totals(0, me, args)
    low = ROWS - CUT
    outs = [((2, CUT, 128), BF16)] * 4 + [((4, low, 128), BF16)] * 2
    keep, one, two, three, near, far = call(pair_body, outs, (own, came), (me,))
    far = along_client(far, 1, 0)
    moved = [along_client(a, 0, d) for d, a in ((1, one), (2, two), (3, three))]
    outs = [((CUT, 128), F32), ((CUT, 128), BF16)] + [((low, 128), BF16)] * 4
    stay, go, kept, one, two, three = call(cross_body, outs, (keep, *moved, near, far), (me,))
    go = along_client(go, 1, 0)
    moved = [along_client(a, 0, d) for d, a in ((1, one), (2, two), (3, three))]
    gate, up, down, gains = call(
        last_body,
        [((128, UNITS), F32), ((128, UNITS), F32), ((UNITS, 128), F32), ((1, 128), F32)],
        (stay, go, kept, *moved),
    )
    return gate, up, down, gains.reshape(128)


def solution(mesh):
    placed = (
        P("client", None, None),
        P("client", None, None),
        P(),
        P(None, "tp"),
        P(None, "tp"),
        P("tp", None),
        P("client", None, "tp"),
    )
    return jax.shard_map(
        on_device,
        mesh=mesh,
        in_specs=placed,
        out_specs=(P("client", "tp"), P("client", "tp"), P("tp", "client"), P("client")),
        check_vma=False,
    )
```

```python
import math

import jax
import jax.numpy as jnp
from jax import lax
from jax.experimental import pallas as pl
from jax.experimental.pallas import tpu as pltpu
from jax.sharding import PartitionSpec as P

D = 2048
FF = 4096
STEPS = 3
RATE = 0.005
LIMIT = 0.5 * math.sqrt(3.0 * D * FF)
TOK = 128
UNITS = 256
BLOCK = 32
LIMIT_BYTES = 20 * 1024 * 1024
FIRST_BYTES = 50 * 1024 * 1024
ROWS = 3 * UNITS + 16
CUT = 496


BF16 = jnp.bfloat16
F32 = jnp.float32


def dot_nn(a, b):
    return jnp.dot(a, b, preferred_element_type=F32)


def dot_nt(a, b):
    return lax.dot_general(a, b, (((1,), (1,)), ((), ())), preferred_element_type=F32)


def call(body, outs, args, scalars=()):
    return pl.pallas_call(
        body,
        out_shape=tuple(jax.ShapeDtypeStruct(s, d) for s, d in outs),
        in_specs=[pl.BlockSpec(memory_space=pltpu.SMEM)] * len(scalars)
        + [pl.BlockSpec(memory_space=pltpu.VMEM)] * len(args),
        out_specs=tuple(pl.BlockSpec(memory_space=pltpu.VMEM) for _ in outs),
        compiler_params=pltpu.CompilerParams(vmem_limit_bytes=LIMIT_BYTES),
    )(*scalars, *args)


def token_block(i):
    return pl.ds(pl.multiple_of(i * BLOCK, BLOCK), BLOCK)


def forward(y, normed, wg, wu, down, past, coefs, act_ref, hid_ref, *part_refs):
    gate = dot_nn(normed, wg[...])
    up = dot_nn(normed, wu[...])
    for (n, g, h, e), a in zip(past, coefs):
        k = (dot_nt(normed, n[...]) * a).astype(BF16)
        gate = gate - dot_nn(k, g[:, :UNITS])
        up = up - dot_nn(k, g[:, UNITS:])
    act_ref[:, :UNITS] = gate
    act_ref[:, UNITS:] = up
    hidden = (gate * jax.nn.sigmoid(gate) * up).astype(BF16)
    hid_ref[...] = hidden
    turned = jnp.concatenate([hid_ref[token_block(y ^ d)] for d in range(4)], axis=0)
    share = dot_nn(turned, down[...])
    for (n, g, h, e), a in zip(past, coefs):
        k = (dot_nt(turned, h[...]) * a).astype(BF16)
        share = share - dot_nn(k, e[...])
    for d in range(4):
        part_refs[d][...] = share[d * BLOCK : (d + 1) * BLOCK].astype(BF16)


def weights_body(me, wg, wu, down, wg_ref, wu_ref, down_ref, sems):
    moves = [(wg, wg_ref), (wu, wu_ref), (down, down_ref)]
    moves = [pltpu.make_async_copy(a, b, sems.at[i]) for i, (a, b) in enumerate(moves)]
    for m in moves:
        m.start()
    for m in moves:
        m.wait()


def in_vmem(me, weights):
    vmem, far = pl.BlockSpec(memory_space=pltpu.VMEM), pl.BlockSpec(memory_space=pltpu.HBM)
    return pl.pallas_call(
        weights_body,
        out_shape=tuple(jax.ShapeDtypeStruct(w.shape, w.dtype) for w in weights),
        in_specs=[pl.BlockSpec(memory_space=pltpu.SMEM), far, far, far],
        out_specs=(vmem, vmem, vmem),
        scratch_shapes=[pltpu.SemaphoreType.DMA((3,))],
        compiler_params=pltpu.CompilerParams(vmem_limit_bytes=FIRST_BYTES),
    )(me, *weights)


def first_body(mine, x, gain, wg, wu, down, scaled_ref, norm_ref, act_ref, hid_ref, *part_refs):
    activ = x[...].astype(F32)
    scaled = activ * lax.rsqrt(jnp.mean(activ * activ, axis=-1, keepdims=True) + 1e-05)
    scaled_ref[...] = scaled
    normed = (scaled * gain[...]).astype(BF16)
    norm_ref[...] = normed
    forward(mine[0] // 4, normed, wg, wu, down, (), (), act_ref, hid_ref, *part_refs)


def sums_of(arrived):
    total = arrived[0].astype(F32)
    for i in range(1, 16):
        total = total + arrived[i].astype(F32)
    grad_gain = jnp.concatenate([total[r : r + 1, :256] for r in range(8)], axis=1)
    squares = jnp.sum(jnp.sum(total[0:3, 256:], axis=0, keepdims=True), axis=1, keepdims=True)
    squares = squares + jnp.sum(grad_gain * grad_gain, axis=1, keepdims=True)
    flagged = total[3:4, 256:257]
    norm = jnp.sqrt(squares + 1e-06)
    factor = jnp.where(flagged < 0.5, LIMIT / jnp.maximum(norm, LIMIT), 0.0)
    return grad_gain, factor


def next_body(step, mine, *refs):
    arrived, gain, gain_total, scaled, wg, wu, down = refs[:7]
    at = 7
    past = [refs[at + 4 * j : at + 4 * j + 4] for j in range(step)]
    at += 4 * step
    old = refs[at : at + step - 1]
    at += step - 1
    factor_ref, gain_ref, total_ref, norm_ref, act_ref, hid_ref = refs[at : at + 6]
    part_refs = refs[at + 6 :]
    grad_gain, factor = sums_of(arrived)
    factor_ref[...] = jnp.broadcast_to(factor, (8, 128))
    new_gain = gain[...] - RATE * factor * grad_gain
    gain_ref[...] = new_gain
    total_ref[...] = gain_total[...] + factor * grad_gain
    normed = (scaled[...] * new_gain).astype(BF16)
    norm_ref[...] = normed
    coefs = [RATE * r[0:1, 0:1] for r in old] + [RATE * factor]
    forward(mine[0] // 4, normed, wg, wu, down, past, coefs, act_ref, hid_ref, *part_refs)


def summed(refs):
    total = refs[0][...].astype(F32)
    for r in refs[1:]:
        total = total + r[...].astype(F32)
    return total


def row_body(*refs):
    refs[-1][...] = summed(refs[:-1]).astype(BF16)


def first_error_body(mine, a, b, c, d, x, t, out_ref, diff_ref):
    rows = token_block(mine[0] // 4)
    diff = x[rows].astype(F32) - t[rows].astype(F32)
    diff_ref[...] = diff
    out_ref[...] = (summed((a, b, c, d)) + diff).astype(BF16)


def error_body(a, b, c, d, diff, out_ref):
    out_ref[...] = (summed((a, b, c, d)) + diff[...]).astype(BF16)


def pieces(value):
    first = value.astype(BF16)
    rest = value - first.astype(F32)
    second = rest.astype(BF16)
    third = (rest - second.astype(F32)).astype(BF16)
    return [first.astype(F32), second.astype(F32), third.astype(F32)]


def back_body(step, flags, mine, *refs):
    errors, (wg, wu, down, scaled, normed, act, hidden) = refs[:4], refs[4:11]
    at = 11
    past = [refs[at + 4 * j : at + 4 * j + 4] for j in range(step)]
    at += 4 * step
    coefs = [RATE * r[0:1, 0:1] for r in refs[at : at + step]]
    at += step
    err_ref, grad_ref, pay_ref = refs[at:]
    for d, came in zip((0, 1, 3, 2), errors):
        err_ref[token_block((mine[0] // 4) ^ d)] = came[...]
    err = err_ref[...]
    hid = hidden[...]
    nrm = normed[...]
    grad_hidden = dot_nt(err, down[...])
    for (n, g, h, e), a in zip(past, coefs):
        k = (dot_nt(err, e[...]) * a).astype(BF16)
        grad_hidden = grad_hidden - dot_nn(k, h[...])
    gate, up = act[:, :UNITS], act[:, UNITS:]
    sig = jax.nn.sigmoid(gate)
    g_gate = (grad_hidden * up * (sig * (1.0 + gate * (1.0 - sig)))).astype(BF16)
    g_up = (grad_hidden * (gate * sig)).astype(BF16)
    grad_ref[:, :UNITS] = g_gate
    grad_ref[:, UNITS:] = g_up
    grads = jnp.concatenate([g_gate, g_up], axis=1)
    grad_normed = dot_nt(g_gate, wg[...]) + dot_nt(g_up, wu[...])
    for (n, g, h, e), a in zip(past, coefs):
        k = (dot_nt(grads, g[...]) * a).astype(BF16)
        grad_normed = grad_normed - dot_nn(k, n[...])
    gain_part = jnp.sum(grad_normed * scaled[...], axis=0, keepdims=True)
    square = dot_nt(nrm, nrm) * dot_nt(grads, grads) + dot_nt(err, err) * dot_nt(hid, hid)
    square = jnp.sum(square, axis=0, keepdims=True)
    flag = jnp.full((1, 128), flags[step].astype(F32))
    tail = jnp.concatenate(pieces(square) + [flag, jnp.zeros((4, 128), F32)], axis=0)
    head = jnp.concatenate([gain_part[:, r * 256 : (r + 1) * 256] for r in range(8)], axis=0)
    packed = jnp.concatenate([head, tail], axis=1).astype(BF16)
    for i in range(16):
        pay_ref[i] = packed


def totals_body(flip, me, *refs):
    arrived, gain_total = refs[:2]
    past = [refs[2 + 4 * j : 6 + 4 * j] for j in range(STEPS)]
    old = refs[2 + 4 * STEPS : 2 + 4 * STEPS + STEPS - 1]
    out_ref, left, gain_row = refs[2 + 4 * STEPS + STEPS - 1 :]
    grad_gain, factor = sums_of(arrived)
    gains = gain_total[...] + factor * grad_gain
    factors = [r[0:1, 0:1] for r in old] + [factor]
    for j, ((n, g, h, e), f) in enumerate(zip(past, factors)):
        left[: 2 * UNITS, j * TOK : (j + 1) * TOK] = (g[...].astype(F32) * f).T.astype(BF16)
        left[2 * UNITS :, j * TOK : (j + 1) * TOK] = (h[...].astype(F32) * f).T.astype(BF16)
    gain_row[...] = gains
    w = lax.rem(me[0] + flip, 2)

    def two_blocks(i, carry):
        for b in (2 * i, 2 * i + 1):
            col = pl.ds(pl.multiple_of((2 * b + w) * 128, 128), 128)
            rows = jnp.concatenate([p[0][:, col] for p in past], axis=0)
            errs = jnp.concatenate([p[3][:, col] for p in past], axis=0)
            out_ref[b, : 2 * UNITS] = dot_nn(left[: 2 * UNITS], rows).astype(BF16)
            out_ref[b, 2 * UNITS : 3 * UNITS] = dot_nn(left[2 * UNITS :], errs).astype(BF16)
            out_ref[b, 3 * UNITS :] = jnp.broadcast_to(gain_row[:, col], (16, 128)).astype(BF16)
        return carry

    lax.fori_loop(0, 4, two_blocks, 0)


def totals(flip, me, args):
    return pl.pallas_call(
        lambda *refs: totals_body(flip, *refs),
        out_shape=jax.ShapeDtypeStruct((8, ROWS, 128), BF16),
        in_specs=[pl.BlockSpec(memory_space=pltpu.SMEM)] + [pl.BlockSpec(memory_space=pltpu.VMEM)] * len(args),
        out_specs=pl.BlockSpec(memory_space=pltpu.VMEM),
        scratch_shapes=[pltpu.VMEM((3 * UNITS, STEPS * TOK), BF16), pltpu.VMEM((1, D), F32)],
        compiler_params=pltpu.CompilerParams(vmem_limit_bytes=LIMIT_BYTES),
    )(me, *args)


def pair_body(me, own, came, *outs):
    x, h = lax.rem(me[0] // 2, 4), me[0] // 8
    for g in range(2):
        for d in range(4):
            i = g * 4 + (x ^ d)
            outs[d][g] = (own[i, :CUT].astype(F32) + came[i, :CUT].astype(F32)).astype(BF16)
    for d in range(2):
        for k in range(4):
            i = lax.rem(h + d, 2) * 4 + k
            outs[4 + d][k] = (own[i, CUT:].astype(F32) + came[i, CUT:].astype(F32)).astype(BF16)


def cross_body(me, keep, one, two, three, near, far, stay_ref, go_ref, *outs):
    x, h = lax.rem(me[0] // 2, 4), me[0] // 8

    def total(g):
        return keep[g].astype(F32) + one[g].astype(F32) + two[g].astype(F32) + three[g].astype(F32)

    stay_ref[...] = total(h)
    go_ref[...] = total(1 - h).astype(BF16)
    for d in range(4):
        i = x ^ d
        outs[d][...] = (near[i].astype(F32) + far[i].astype(F32)).astype(BF16)


def last_body(stay, came, a, b, c, d, gate_ref, up_ref, down_ref, gain_ref):
    top = (stay[...] + came[...].astype(F32)) * (1.0 / 16.0)
    total = jnp.concatenate([top, summed((a, b, c, d)) * (1.0 / 16.0)], axis=0)
    gate_ref[...] = total[:UNITS].T
    up_ref[...] = total[UNITS : 2 * UNITS].T
    down_ref[...] = total[2 * UNITS : 3 * UNITS]
    gain_ref[...] = total[3 * UNITS : 3 * UNITS + 1]


def client_perm(dh, dx, dc):
    return [
        (h * 8 + x * 2 + c, ((h + dh) % 2) * 8 + (x ^ dx) * 2 + (c + dc) % 2)
        for h in range(2)
        for x in range(4)
        for c in range(2)
    ]


def along_client(array, dh, dx):
    return lax.ppermute(array, "client", client_perm(dh, dx, 0))


def along_y(array, d):
    pairs = [(y * 4 + z, (y ^ d) * 4 + z) for y in range(4) for z in range(4)]
    return lax.ppermute(array, "tp", pairs)


def along_z(array, d):
    pairs = [(y * 4 + z, y * 4 + (z ^ d)) for y in range(4) for z in range(4)]
    return lax.ppermute(array, "tp", pairs)


def to_all(array, axis):
    return lax.all_to_all(array, axis, 0, 0, tiled=True)


def on_device(inputs, targets, norm_gain, gate_weight, up_weight, down_weight, overflow):
    mine = lax.axis_index("tp").reshape(1)
    me = lax.axis_index("client").reshape(1)
    flags = overflow.reshape(STEPS)
    gain = norm_gain.reshape(1, D)
    gain_total = jnp.zeros((1, D), F32)
    weights = tuple(in_vmem(me, (gate_weight, up_weight, down_weight)))
    row = ((1, D), F32)
    made = [((TOK, D), BF16), ((TOK, 2 * UNITS), F32), ((TOK, UNITS), BF16)] + [((BLOCK, D), BF16)] * 4
    past, factors, arrived, diff = [], [], None, None
    for step in range(STEPS):
        flat = [r for p in past for r in p]
        if step == 0:
            scaled, normed, act, hidden, *parts = call(
                first_body, [((TOK, D), F32)] + made, (inputs[0], gain) + weights, (mine,)
            )
        else:
            body = lambda *refs, step=step: next_body(step, *refs)
            factor, gain, gain_total, normed, act, hidden, *parts = call(
                body,
                [((8, 128), F32), row, row] + made,
                (arrived, gain, gain_total, scaled) + weights + tuple(flat + factors),
                (mine,),
            )
            factors = factors + [factor]
        block = ((BLOCK, D), BF16)
        (rows,) = call(row_body, [block], (parts[0], *[along_y(parts[d], d) for d in (2, 3, 1)]))
        came = [along_z(rows, d) for d in (1, 2, 3)]
        if step == 0:
            error, diff = call(first_error_body, [block, ((BLOCK, D), F32)], (rows, *came, inputs[0], targets[0]), (mine,))
        else:
            (error,) = call(error_body, [block], (rows, *came, diff))
        one, three, two = [along_y(error, d) for d in (1, 3, 2)]
        errors = (error, one, three, two)
        body = lambda *refs, step=step: back_body(step, *refs)
        error, grads, pay = call(
            body,
            [((TOK, D), BF16), ((TOK, 2 * UNITS), BF16), ((16, 8, 384), BF16)],
            errors + weights + (scaled, normed, act, hidden) + tuple(flat + factors),
            (flags, mine),
        )
        arrived = to_all(pay, "tp")
        past = past + [(normed, grads, hidden, error)]

    flat = [r for p in past for r in p]
    args = (arrived, gain_total, *flat, *factors)
    other = totals(1, me, args)
    came = lax.ppermute(other, "client", client_perm(0, 0, 1))
    own = totals(0, me, args)
    low = ROWS - CUT
    outs = [((2, CUT, 128), BF16)] * 4 + [((4, low, 128), BF16)] * 2
    keep, one, two, three, near, far = call(pair_body, outs, (own, came), (me,))
    far = along_client(far, 1, 0)
    moved = [along_client(a, 0, d) for d, a in ((2, two), (1, one), (3, three))]
    outs = [((CUT, 128), F32), ((CUT, 128), BF16)] + [((low, 128), BF16)] * 4
    stay, go, kept, one, two, three = call(cross_body, outs, (keep, *moved, near, far), (me,))
    go = along_client(go, 1, 0)
    moved = [along_client(a, 0, d) for d, a in ((2, two), (1, one), (3, three))]
    gate, up, down, gains = call(
        last_body,
        [((128, UNITS), F32), ((128, UNITS), F32), ((UNITS, 128), F32), ((1, 128), F32)],
        (stay, go, kept, *moved),
    )
    return gate, up, down, gains.reshape(128)


def solution(mesh):
    placed = (
        P("client", None, None),
        P("client", None, None),
        P(),
        P(None, "tp"),
        P(None, "tp"),
        P("tp", None),
        P("client", None, "tp"),
    )
    return jax.shard_map(
        on_device,
        mesh=mesh,
        in_specs=placed,
        out_specs=(P("client", "tp"), P("client", "tp"), P("tp", "client"), P("client")),
        check_vma=False,
    )
```

```python
import math

import jax
import jax.numpy as jnp
from jax import lax
from jax.experimental import pallas as pl
from jax.experimental.pallas import tpu as pltpu
from jax.sharding import PartitionSpec as P

D = 2048
FF = 4096
STEPS = 3
RATE = 0.005
LIMIT = 0.5 * math.sqrt(3.0 * D * FF)
TOK = 128
UNITS = 256
BLOCK = 32
LIMIT_BYTES = 20 * 1024 * 1024
FIRST_BYTES = 50 * 1024 * 1024
ROWS = 3 * UNITS + 16
CUT = 496


BF16 = jnp.bfloat16
F32 = jnp.float32


def dot_nn(a, b):
    return jnp.dot(a, b, preferred_element_type=F32)


def dot_nt(a, b):
    return lax.dot_general(a, b, (((1,), (1,)), ((), ())), preferred_element_type=F32)


def call(body, outs, args, scalars=()):
    return pl.pallas_call(
        body,
        out_shape=tuple(jax.ShapeDtypeStruct(s, d) for s, d in outs),
        in_specs=[pl.BlockSpec(memory_space=pltpu.SMEM)] * len(scalars)
        + [pl.BlockSpec(memory_space=pltpu.VMEM)] * len(args),
        out_specs=tuple(pl.BlockSpec(memory_space=pltpu.VMEM) for _ in outs),
        compiler_params=pltpu.CompilerParams(vmem_limit_bytes=LIMIT_BYTES),
    )(*scalars, *args)


def token_block(i):
    return pl.ds(pl.multiple_of(i * BLOCK, BLOCK), BLOCK)


def forward(y, normed, wg, wu, down, past, coefs, act_ref, hid_ref, *part_refs):
    gate = dot_nn(normed, wg[...])
    up = dot_nn(normed, wu[...])
    for (n, g, h, e), a in zip(past, coefs):
        k = (dot_nt(normed, n[...]) * a).astype(BF16)
        gate = gate - dot_nn(k, g[:, :UNITS])
        up = up - dot_nn(k, g[:, UNITS:])
    act_ref[:, :UNITS] = gate
    act_ref[:, UNITS:] = up
    hidden = (gate * jax.nn.sigmoid(gate) * up).astype(BF16)
    hid_ref[...] = hidden
    turned = jnp.concatenate([hid_ref[token_block(y ^ d)] for d in range(4)], axis=0)
    share = dot_nn(turned, down[...])
    for (n, g, h, e), a in zip(past, coefs):
        k = (dot_nt(turned, h[...]) * a).astype(BF16)
        share = share - dot_nn(k, e[...])
    for d in range(4):
        part_refs[d][...] = share[d * BLOCK : (d + 1) * BLOCK].astype(BF16)


def weights_body(me, wg, wu, down, wg_ref, wu_ref, down_ref, sems):
    moves = [(wg, wg_ref), (wu, wu_ref), (down, down_ref)]
    moves = [pltpu.make_async_copy(a, b, sems.at[i]) for i, (a, b) in enumerate(moves)]
    for m in moves:
        m.start()
    for m in moves:
        m.wait()


def in_vmem(me, weights):
    vmem, far = pl.BlockSpec(memory_space=pltpu.VMEM), pl.BlockSpec(memory_space=pltpu.HBM)
    return pl.pallas_call(
        weights_body,
        out_shape=tuple(jax.ShapeDtypeStruct(w.shape, w.dtype) for w in weights),
        in_specs=[pl.BlockSpec(memory_space=pltpu.SMEM), far, far, far],
        out_specs=(vmem, vmem, vmem),
        scratch_shapes=[pltpu.SemaphoreType.DMA((3,))],
        compiler_params=pltpu.CompilerParams(vmem_limit_bytes=FIRST_BYTES),
    )(me, *weights)


def first_body(mine, x, gain, wg, wu, down, scaled_ref, norm_ref, act_ref, hid_ref, *part_refs):
    activ = x[...].astype(F32)
    scaled = activ * lax.rsqrt(jnp.mean(activ * activ, axis=-1, keepdims=True) + 1e-05)
    scaled_ref[...] = scaled
    normed = (scaled * gain[...]).astype(BF16)
    norm_ref[...] = normed
    forward(mine[0] // 4, normed, wg, wu, down, (), (), act_ref, hid_ref, *part_refs)


def sums_of(arrived):
    total = arrived[0].astype(F32)
    for i in range(1, 16):
        total = total + arrived[i].astype(F32)
    grad_gain = jnp.concatenate([total[r : r + 1, :256] for r in range(8)], axis=1)
    squares = jnp.sum(jnp.sum(total[0:3, 256:], axis=0, keepdims=True), axis=1, keepdims=True)
    squares = squares + jnp.sum(grad_gain * grad_gain, axis=1, keepdims=True)
    flagged = total[3:4, 256:257]
    norm = jnp.sqrt(squares + 1e-06)
    factor = jnp.where(flagged < 0.5, LIMIT / jnp.maximum(norm, LIMIT), 0.0)
    return grad_gain, factor


def next_body(step, mine, *refs):
    arrived, gain, gain_total, scaled, wg, wu, down = refs[:7]
    at = 7
    past = [refs[at + 4 * j : at + 4 * j + 4] for j in range(step)]
    at += 4 * step
    old = refs[at : at + step - 1]
    at += step - 1
    factor_ref, gain_ref, total_ref, norm_ref, act_ref, hid_ref = refs[at : at + 6]
    part_refs = refs[at + 6 :]
    grad_gain, factor = sums_of(arrived)
    factor_ref[...] = jnp.broadcast_to(factor, (8, 128))
    new_gain = gain[...] - RATE * factor * grad_gain
    gain_ref[...] = new_gain
    total_ref[...] = gain_total[...] + factor * grad_gain
    normed = (scaled[...] * new_gain).astype(BF16)
    norm_ref[...] = normed
    coefs = [RATE * r[0:1, 0:1] for r in old] + [RATE * factor]
    forward(mine[0] // 4, normed, wg, wu, down, past, coefs, act_ref, hid_ref, *part_refs)


def summed(refs):
    total = refs[0][...].astype(F32)
    for r in refs[1:]:
        total = total + r[...].astype(F32)
    return total


def row_body(*refs):
    refs[-1][...] = summed(refs[:-1]).astype(BF16)


def first_error_body(mine, a, b, c, d, x, t, out_ref, diff_ref):
    rows = token_block(mine[0] // 4)
    diff = x[rows].astype(F32) - t[rows].astype(F32)
    diff_ref[...] = diff
    out_ref[...] = (summed((a, b, c, d)) + diff).astype(BF16)


def error_body(a, b, c, d, diff, *rest):
    out_ref = rest[-1]
    out_ref[...] = (summed((a, b, c, d)) + diff[...]).astype(BF16)


def pieces(value):
    first = value.astype(BF16)
    rest = value - first.astype(F32)
    second = rest.astype(BF16)
    third = (rest - second.astype(F32)).astype(BF16)
    return [first.astype(F32), second.astype(F32), third.astype(F32)]


def ahead_body(normed, act, hidden, nn_ref, hh_ref, slope_ref):
    nn_ref[...] = dot_nt(normed[...], normed[...])
    hh_ref[...] = dot_nt(hidden[...], hidden[...])
    gate, up = act[:, :UNITS], act[:, UNITS:]
    sig = jax.nn.sigmoid(gate)
    slope_ref[:, :UNITS] = up * (sig * (1.0 + gate * (1.0 - sig)))
    slope_ref[:, UNITS:] = gate * sig


def back_body(step, flags, mine, *refs):
    errors, (wg, wu, down, scaled, nn, hh, slope) = refs[:4], refs[4:11]
    at = 11
    past = [refs[at + 4 * j : at + 4 * j + 4] for j in range(step)]
    at += 4 * step
    coefs = [RATE * r[0:1, 0:1] for r in refs[at : at + step]]
    at += step
    err_ref, grad_ref, pay_ref = refs[at:]
    for d, came in zip((0, 1, 3, 2), errors):
        err_ref[token_block((mine[0] // 4) ^ d)] = came[...]
    err = err_ref[...]
    grad_hidden = dot_nt(err, down[...])
    for (n, g, h, e), a in zip(past, coefs):
        k = (dot_nt(err, e[...]) * a).astype(BF16)
        grad_hidden = grad_hidden - dot_nn(k, h[...])
    g_gate = (grad_hidden * slope[:, :UNITS]).astype(BF16)
    g_up = (grad_hidden * slope[:, UNITS:]).astype(BF16)
    grad_ref[:, :UNITS] = g_gate
    grad_ref[:, UNITS:] = g_up
    grads = jnp.concatenate([g_gate, g_up], axis=1)
    grad_normed = dot_nt(g_gate, wg[...]) + dot_nt(g_up, wu[...])
    for (n, g, h, e), a in zip(past, coefs):
        k = (dot_nt(grads, g[...]) * a).astype(BF16)
        grad_normed = grad_normed - dot_nn(k, n[...])
    gain_part = jnp.sum(grad_normed * scaled[...], axis=0, keepdims=True)
    square = nn[...] * dot_nt(grads, grads) + dot_nt(err, err) * hh[...]
    square = jnp.sum(square, axis=0, keepdims=True)
    flag = jnp.full((1, 128), flags[step].astype(F32))
    tail = jnp.concatenate(pieces(square) + [flag, jnp.zeros((4, 128), F32)], axis=0)
    head = jnp.concatenate([gain_part[:, r * 256 : (r + 1) * 256] for r in range(8)], axis=0)
    packed = jnp.concatenate([head, tail], axis=1).astype(BF16)
    for i in range(16):
        pay_ref[i] = packed


def early_body(*refs):
    past = [refs[4 * j : 4 * j + 4] for j in range(STEPS - 1)]
    factors = refs[4 * (STEPS - 1) : 5 * (STEPS - 1)]
    out_ref, left = refs[5 * (STEPS - 1) :]
    for j, ((n, g, h, e), r) in enumerate(zip(past, factors)):
        f = r[0:1, 0:1]
        left[: 2 * UNITS, j * TOK : (j + 1) * TOK] = (g[...].astype(F32) * f).T.astype(BF16)
        left[2 * UNITS :, j * TOK : (j + 1) * TOK] = (h[...].astype(F32) * f).T.astype(BF16)

    def two_blocks(i, carry):
        col = pl.ds(pl.multiple_of(i * 256, 256), 256)
        rows = jnp.concatenate([p[0][:, col] for p in past], axis=0)
        errs = jnp.concatenate([p[3][:, col] for p in past], axis=0)
        top, low = dot_nn(left[: 2 * UNITS], rows), dot_nn(left[2 * UNITS :], errs)
        for k in range(2):
            out_ref[2 * i + k, : 2 * UNITS] = top[:, k * 128 : (k + 1) * 128]
            out_ref[2 * i + k, 2 * UNITS :] = low[:, k * 128 : (k + 1) * 128]
        return carry

    lax.fori_loop(0, 8, two_blocks, 0)


def early(args):
    vmem = pl.BlockSpec(memory_space=pltpu.VMEM)
    return pl.pallas_call(
        early_body,
        out_shape=jax.ShapeDtypeStruct((16, 3 * UNITS, 128), F32),
        in_specs=[vmem] * len(args),
        out_specs=vmem,
        scratch_shapes=[pltpu.VMEM((3 * UNITS, (STEPS - 1) * TOK), BF16)],
        compiler_params=pltpu.CompilerParams(vmem_limit_bytes=LIMIT_BYTES),
    )(*args)


def totals_body(flip, me, arrived, gain_total, before, n, g, h, e, out_ref, left, gain_row):
    grad_gain, factor = sums_of(arrived)
    gain_row[...] = gain_total[...] + factor * grad_gain
    left[: 2 * UNITS] = (g[...].astype(F32) * factor).T.astype(BF16)
    left[2 * UNITS :] = (h[...].astype(F32) * factor).T.astype(BF16)
    w = lax.rem(me[0] + flip, 2)
    for b in range(8):
        i = 2 * b + w
        col = pl.ds(pl.multiple_of(i * 128, 128), 128)
        top = before[i, : 2 * UNITS] + dot_nn(left[: 2 * UNITS], n[:, col])
        low = before[i, 2 * UNITS :] + dot_nn(left[2 * UNITS :], e[:, col])
        out_ref[b, : 2 * UNITS] = top.astype(BF16)
        out_ref[b, 2 * UNITS : 3 * UNITS] = low.astype(BF16)
        out_ref[b, 3 * UNITS :] = jnp.broadcast_to(gain_row[:, col], (16, 128)).astype(BF16)


def totals(flip, me, args):
    return pl.pallas_call(
        lambda *refs: totals_body(flip, *refs),
        out_shape=jax.ShapeDtypeStruct((8, ROWS, 128), BF16),
        in_specs=[pl.BlockSpec(memory_space=pltpu.SMEM)] + [pl.BlockSpec(memory_space=pltpu.VMEM)] * len(args),
        out_specs=pl.BlockSpec(memory_space=pltpu.VMEM),
        scratch_shapes=[pltpu.VMEM((3 * UNITS, TOK), BF16), pltpu.VMEM((1, D), F32)],
        compiler_params=pltpu.CompilerParams(vmem_limit_bytes=LIMIT_BYTES),
    )(me, *args)


def pair_body(me, own, came, *outs):
    x, h = lax.rem(me[0] // 2, 4), me[0] // 8
    for g in range(2):
        for d in range(4):
            i = g * 4 + (x ^ d)
            outs[d][g] = (own[i, :CUT].astype(F32) + came[i, :CUT].astype(F32)).astype(BF16)
    for d in range(2):
        for k in range(4):
            i = lax.rem(h + d, 2) * 4 + k
            outs[4 + d][k] = (own[i, CUT:].astype(F32) + came[i, CUT:].astype(F32)).astype(BF16)


def cross_body(me, keep, one, two, three, near, far, stay_ref, go_ref, *outs):
    x, h = lax.rem(me[0] // 2, 4), me[0] // 8

    def total(g):
        return keep[g].astype(F32) + one[g].astype(F32) + two[g].astype(F32) + three[g].astype(F32)

    stay_ref[...] = total(h)
    go_ref[...] = total(1 - h).astype(BF16)
    for d in range(4):
        i = x ^ d
        outs[d][...] = (near[i].astype(F32) + far[i].astype(F32)).astype(BF16)


def last_body(stay, came, a, b, c, d, gate_ref, up_ref, down_ref, gain_ref):
    top = (stay[...] + came[...].astype(F32)) * (1.0 / 16.0)
    total = jnp.concatenate([top, summed((a, b, c, d)) * (1.0 / 16.0)], axis=0)
    gate_ref[...] = total[:UNITS].T
    up_ref[...] = total[UNITS : 2 * UNITS].T
    down_ref[...] = total[2 * UNITS : 3 * UNITS]
    gain_ref[...] = total[3 * UNITS : 3 * UNITS + 1]


def client_perm(dh, dx, dc):
    return [
        (h * 8 + x * 2 + c, ((h + dh) % 2) * 8 + (x ^ dx) * 2 + (c + dc) % 2)
        for h in range(2)
        for x in range(4)
        for c in range(2)
    ]


def along_client(array, dh, dx):
    return lax.ppermute(array, "client", client_perm(dh, dx, 0))


def along_y(array, d):
    pairs = [(y * 4 + z, (y ^ d) * 4 + z) for y in range(4) for z in range(4)]
    return lax.ppermute(array, "tp", pairs)


def along_z(array, d):
    pairs = [(y * 4 + z, y * 4 + (z + d) % 4) for y in range(4) for z in range(4)]
    return lax.ppermute(array, "tp", pairs)


def to_all(array, axis):
    return lax.all_to_all(array, axis, 0, 0, tiled=True)


def on_device(inputs, targets, norm_gain, gate_weight, up_weight, down_weight, overflow):
    mine = lax.axis_index("tp").reshape(1)
    me = lax.axis_index("client").reshape(1)
    flags = overflow.reshape(STEPS)
    gain = norm_gain.reshape(1, D)
    gain_total = jnp.zeros((1, D), F32)
    weights = tuple(in_vmem(me, (gate_weight, up_weight, down_weight)))
    row = ((1, D), F32)
    made = [((TOK, D), BF16), ((TOK, 2 * UNITS), F32), ((TOK, UNITS), BF16)] + [((BLOCK, D), BF16)] * 4
    past, factors, arrived, diff = [], [], None, None
    for step in range(STEPS):
        flat = [r for p in past for r in p]
        if step == 0:
            scaled, normed, act, hidden, *parts = call(
                first_body, [((TOK, D), F32)] + made, (inputs[0], gain) + weights, (mine,)
            )
        else:
            body = lambda *refs, step=step: next_body(step, *refs)
            factor, gain, gain_total, normed, act, hidden, *parts = call(
                body,
                [((8, 128), F32), row, row] + made,
                (arrived, gain, gain_total, scaled) + weights + tuple(flat + factors),
                (mine,),
            )
            factors = factors + [factor]
        block = ((BLOCK, D), BF16)
        square = ((TOK, TOK), F32)
        ahead = call(ahead_body, [square, square, ((TOK, 2 * UNITS), F32)], (normed, act, hidden))
        if step == STEPS - 1:
            before = early((*flat, *factors))
        (rows,) = call(row_body, [block], (parts[0], *[along_y(parts[d], d) for d in (2, 3, 1)]))
        came = [along_z(rows, d) for d in (1, 2, 3)]
        if step == 0:
            error, diff = call(first_error_body, [block, ((BLOCK, D), F32)], (rows, *came, inputs[0], targets[0]), (mine,))
        else:
            done = (before,) if step == STEPS - 1 else ()
            (error,) = call(error_body, [block], (rows, *came, diff, *done))
        one, three, two = [along_y(error, d) for d in (1, 3, 2)]
        errors = (error, one, three, two)
        body = lambda *refs, step=step: back_body(step, *refs)
        error, grads, pay = call(
            body,
            [((TOK, D), BF16), ((TOK, 2 * UNITS), BF16), ((16, 8, 384), BF16)],
            errors + weights + (scaled, *ahead) + tuple(flat + factors),
            (flags, mine),
        )
        arrived = to_all(pay, "tp")
        past = past + [(normed, grads, hidden, error)]

    args = (arrived, gain_total, before, *past[-1])
    other = totals(1, me, args)
    came = lax.ppermute(other, "client", client_perm(0, 0, 1))
    own = totals(0, me, args)
    low = ROWS - CUT
    outs = [((2, CUT, 128), BF16)] * 4 + [((4, low, 128), BF16)] * 2
    keep, one, two, three, near, far = call(pair_body, outs, (own, came), (me,))
    far = along_client(far, 1, 0)
    moved = [along_client(a, 0, d) for d, a in ((2, two), (1, one), (3, three))]
    outs = [((CUT, 128), F32), ((CUT, 128), BF16)] + [((low, 128), BF16)] * 4
    stay, go, kept, one, two, three = call(cross_body, outs, (keep, *moved, near, far), (me,))
    go = along_client(go, 1, 0)
    moved = [along_client(a, 0, d) for d, a in ((2, two), (1, one), (3, three))]
    gate, up, down, gains = call(
        last_body,
        [((128, UNITS), F32), ((128, UNITS), F32), ((UNITS, 128), F32), ((1, 128), F32)],
        (stay, go, kept, *moved),
    )
    return gate, up, down, gains.reshape(128)


def solution(mesh):
    placed = (
        P("client", None, None),
        P("client", None, None),
        P(),
        P(None, "tp"),
        P(None, "tp"),
        P("tp", None),
        P("client", None, "tp"),
    )
    return jax.shard_map(
        on_device,
        mesh=mesh,
        in_specs=placed,
        out_specs=(P("client", "tp"), P("client", "tp"), P("tp", "client"), P("client")),
        check_vma=False,
    )
```

```python
import math

import jax
import jax.numpy as jnp
from jax import lax
from jax.experimental import pallas as pl
from jax.experimental.pallas import tpu as pltpu
from jax.sharding import PartitionSpec as P

D = 2048
FF = 4096
STEPS = 3
RATE = 0.005
LIMIT = 0.5 * math.sqrt(3.0 * D * FF)
TOK = 128
UNITS = 256
BLOCK = 32
LIMIT_BYTES = 20 * 1024 * 1024
FIRST_BYTES = 50 * 1024 * 1024
ROWS = 3 * UNITS + 16
CUT = 448


BF16 = jnp.bfloat16
F32 = jnp.float32


def dot_nn(a, b):
    return jnp.dot(a, b, preferred_element_type=F32)


def dot_nt(a, b):
    return lax.dot_general(a, b, (((1,), (1,)), ((), ())), preferred_element_type=F32)


def call(body, outs, args, scalars=()):
    return pl.pallas_call(
        body,
        out_shape=tuple(jax.ShapeDtypeStruct(s, d) for s, d in outs),
        in_specs=[pl.BlockSpec(memory_space=pltpu.SMEM)] * len(scalars)
        + [pl.BlockSpec(memory_space=pltpu.VMEM)] * len(args),
        out_specs=tuple(pl.BlockSpec(memory_space=pltpu.VMEM) for _ in outs),
        compiler_params=pltpu.CompilerParams(vmem_limit_bytes=LIMIT_BYTES),
    )(*scalars, *args)


def token_block(i):
    return pl.ds(pl.multiple_of(i * BLOCK, BLOCK), BLOCK)


def forward(y, normed, wg, wu, down, past, coefs, act_ref, hid_ref, *part_refs):
    gate = dot_nn(normed, wg[...])
    up = dot_nn(normed, wu[...])
    for (n, g, h, e), a in zip(past, coefs):
        k = (dot_nt(normed, n[...]) * a).astype(BF16)
        gate = gate - dot_nn(k, g[:, :UNITS])
        up = up - dot_nn(k, g[:, UNITS:])
    act_ref[:, :UNITS] = gate
    act_ref[:, UNITS:] = up
    hidden = (gate * jax.nn.sigmoid(gate) * up).astype(BF16)
    hid_ref[...] = hidden
    turned = jnp.concatenate([hid_ref[token_block(y ^ d)] for d in range(4)], axis=0)
    share = dot_nn(turned, down[...])
    for (n, g, h, e), a in zip(past, coefs):
        k = (dot_nt(turned, h[...]) * a).astype(BF16)
        share = share - dot_nn(k, e[...])
    for d in range(4):
        part_refs[d][...] = share[d * BLOCK : (d + 1) * BLOCK].astype(BF16)


def weights_body(me, wg, wu, down, wg_ref, wu_ref, down_ref, sems):
    moves = [(wg, wg_ref), (wu, wu_ref), (down, down_ref)]
    moves = [pltpu.make_async_copy(a, b, sems.at[i]) for i, (a, b) in enumerate(moves)]
    for m in moves:
        m.start()
    for m in moves:
        m.wait()


def in_vmem(me, weights):
    vmem, far = pl.BlockSpec(memory_space=pltpu.VMEM), pl.BlockSpec(memory_space=pltpu.HBM)
    return pl.pallas_call(
        weights_body,
        out_shape=tuple(jax.ShapeDtypeStruct(w.shape, w.dtype) for w in weights),
        in_specs=[pl.BlockSpec(memory_space=pltpu.SMEM), far, far, far],
        out_specs=(vmem, vmem, vmem),
        scratch_shapes=[pltpu.SemaphoreType.DMA((3,))],
        compiler_params=pltpu.CompilerParams(vmem_limit_bytes=FIRST_BYTES),
    )(me, *weights)


def first_body(mine, x, gain, wg, wu, down, scaled_ref, norm_ref, act_ref, hid_ref, *part_refs):
    activ = x[...].astype(F32)
    scaled = activ * lax.rsqrt(jnp.mean(activ * activ, axis=-1, keepdims=True) + 1e-05)
    scaled_ref[...] = scaled
    normed = (scaled * gain[...]).astype(BF16)
    norm_ref[...] = normed
    forward(mine[0] // 4, normed, wg, wu, down, (), (), act_ref, hid_ref, *part_refs)


def sums_of(arrived):
    total = arrived[0].astype(F32)
    for i in range(1, 16):
        total = total + arrived[i].astype(F32)
    grad_gain = jnp.concatenate([total[r : r + 1, :256] for r in range(8)], axis=1)
    squares = jnp.sum(jnp.sum(total[0:3, 256:], axis=0, keepdims=True), axis=1, keepdims=True)
    squares = squares + jnp.sum(grad_gain * grad_gain, axis=1, keepdims=True)
    flagged = total[3:4, 256:257]
    norm = jnp.sqrt(squares + 1e-06)
    factor = jnp.where(flagged < 0.5, LIMIT / jnp.maximum(norm, LIMIT), 0.0)
    return grad_gain, factor


def next_body(step, mine, *refs):
    arrived, gain, gain_total, scaled, wg, wu, down = refs[:7]
    at = 7
    past = [refs[at + 4 * j : at + 4 * j + 4] for j in range(step)]
    at += 4 * step
    old = refs[at : at + step - 1]
    at += step - 1
    factor_ref, gain_ref, total_ref, norm_ref, act_ref, hid_ref = refs[at : at + 6]
    part_refs = refs[at + 6 :]
    grad_gain, factor = sums_of(arrived)
    factor_ref[...] = jnp.broadcast_to(factor, (8, 128))
    new_gain = gain[...] - RATE * factor * grad_gain
    gain_ref[...] = new_gain
    total_ref[...] = gain_total[...] + factor * grad_gain
    normed = (scaled[...] * new_gain).astype(BF16)
    norm_ref[...] = normed
    coefs = [RATE * r[0:1, 0:1] for r in old] + [RATE * factor]
    forward(mine[0] // 4, normed, wg, wu, down, past, coefs, act_ref, hid_ref, *part_refs)


def summed(refs):
    total = refs[0][...].astype(F32)
    for r in refs[1:]:
        total = total + r[...].astype(F32)
    return total


def row_body(*refs):
    refs[-1][...] = summed(refs[:-1]).astype(BF16)


def first_error_body(mine, a, b, c, d, x, t, out_ref, diff_ref):
    rows = token_block(mine[0] // 4)
    diff = x[rows].astype(F32) - t[rows].astype(F32)
    diff_ref[...] = diff
    out_ref[...] = (summed((a, b, c, d)) + diff).astype(BF16)


def error_body(a, b, c, d, diff, *rest):
    out_ref = rest[-1]
    out_ref[...] = (summed((a, b, c, d)) + diff[...]).astype(BF16)


def pieces(value):
    first = value.astype(BF16)
    rest = value - first.astype(F32)
    second = rest.astype(BF16)
    third = (rest - second.astype(F32)).astype(BF16)
    return [first.astype(F32), second.astype(F32), third.astype(F32)]


def ahead_body(normed, act, hidden, nn_ref, hh_ref, slope_ref):
    nn_ref[...] = dot_nt(normed[...], normed[...])
    hh_ref[...] = dot_nt(hidden[...], hidden[...])
    gate, up = act[:, :UNITS], act[:, UNITS:]
    sig = jax.nn.sigmoid(gate)
    slope_ref[:, :UNITS] = up * (sig * (1.0 + gate * (1.0 - sig)))
    slope_ref[:, UNITS:] = gate * sig


def back_body(step, flags, mine, *refs):
    errors, (wg, wu, down, scaled, nn, hh, slope) = refs[:4], refs[4:11]
    at = 11
    past = [refs[at + 4 * j : at + 4 * j + 4] for j in range(step)]
    at += 4 * step
    coefs = [RATE * r[0:1, 0:1] for r in refs[at : at + step]]
    at += step
    err_ref, grad_ref, pay_ref = refs[at:]
    for d, came in zip((0, 1, 3, 2), errors):
        err_ref[token_block((mine[0] // 4) ^ d)] = came[...]
    err = err_ref[...]
    grad_hidden = dot_nt(err, down[...])
    for (n, g, h, e), a in zip(past, coefs):
        k = (dot_nt(err, e[...]) * a).astype(BF16)
        grad_hidden = grad_hidden - dot_nn(k, h[...])
    g_gate = (grad_hidden * slope[:, :UNITS]).astype(BF16)
    g_up = (grad_hidden * slope[:, UNITS:]).astype(BF16)
    grad_ref[:, :UNITS] = g_gate
    grad_ref[:, UNITS:] = g_up
    grads = jnp.concatenate([g_gate, g_up], axis=1)
    grad_normed = dot_nt(g_gate, wg[...]) + dot_nt(g_up, wu[...])
    for (n, g, h, e), a in zip(past, coefs):
        k = (dot_nt(grads, g[...]) * a).astype(BF16)
        grad_normed = grad_normed - dot_nn(k, n[...])
    gain_part = jnp.sum(grad_normed * scaled[...], axis=0, keepdims=True)
    square = nn[...] * dot_nt(grads, grads) + dot_nt(err, err) * hh[...]
    square = jnp.sum(square, axis=0, keepdims=True)
    flag = jnp.full((1, 128), flags[step].astype(F32))
    tail = jnp.concatenate(pieces(square) + [flag, jnp.zeros((4, 128), F32)], axis=0)
    head = jnp.concatenate([gain_part[:, r * 256 : (r + 1) * 256] for r in range(8)], axis=0)
    packed = jnp.concatenate([head, tail], axis=1).astype(BF16)
    for i in range(16):
        pay_ref[i] = packed


def early_body(*refs):
    past = [refs[4 * j : 4 * j + 4] for j in range(STEPS - 1)]
    factors = refs[4 * (STEPS - 1) : 5 * (STEPS - 1)]
    out_ref, left = refs[5 * (STEPS - 1) :]
    for j, ((n, g, h, e), r) in enumerate(zip(past, factors)):
        f = r[0:1, 0:1]
        left[: 2 * UNITS, j * TOK : (j + 1) * TOK] = (g[...].astype(F32) * f).T.astype(BF16)
        left[2 * UNITS :, j * TOK : (j + 1) * TOK] = (h[...].astype(F32) * f).T.astype(BF16)

    def two_blocks(i, carry):
        col = pl.ds(pl.multiple_of(i * 256, 256), 256)
        rows = jnp.concatenate([p[0][:, col] for p in past], axis=0)
        errs = jnp.concatenate([p[3][:, col] for p in past], axis=0)
        top, low = dot_nn(left[: 2 * UNITS], rows), dot_nn(left[2 * UNITS :], errs)
        for k in range(2):
            out_ref[2 * i + k, : 2 * UNITS] = top[:, k * 128 : (k + 1) * 128]
            out_ref[2 * i + k, 2 * UNITS :] = low[:, k * 128 : (k + 1) * 128]
        return carry

    lax.fori_loop(0, 8, two_blocks, 0)


def early(args):
    vmem = pl.BlockSpec(memory_space=pltpu.VMEM)
    return pl.pallas_call(
        early_body,
        out_shape=jax.ShapeDtypeStruct((16, 3 * UNITS, 128), F32),
        in_specs=[vmem] * len(args),
        out_specs=vmem,
        scratch_shapes=[pltpu.VMEM((3 * UNITS, (STEPS - 1) * TOK), BF16)],
        compiler_params=pltpu.CompilerParams(vmem_limit_bytes=LIMIT_BYTES),
    )(*args)


def totals_body(flip, me, arrived, gain_total, before, n, g, h, e, out_ref, left, gain_row):
    grad_gain, factor = sums_of(arrived)
    gain_row[...] = gain_total[...] + factor * grad_gain
    left[: 2 * UNITS] = (g[...].astype(F32) * factor).T.astype(BF16)
    left[2 * UNITS :] = (h[...].astype(F32) * factor).T.astype(BF16)
    w = lax.rem(me[0] + flip, 2)
    for b in range(8):
        i = 2 * b + w
        col = pl.ds(pl.multiple_of(i * 128, 128), 128)
        top = before[i, : 2 * UNITS] + dot_nn(left[: 2 * UNITS], n[:, col])
        low = before[i, 2 * UNITS :] + dot_nn(left[2 * UNITS :], e[:, col])
        out_ref[b, : 2 * UNITS] = top.astype(BF16)
        out_ref[b, 2 * UNITS : 3 * UNITS] = low.astype(BF16)
        out_ref[b, 3 * UNITS :] = jnp.broadcast_to(gain_row[:, col], (16, 128)).astype(BF16)


def totals(flip, me, args):
    return pl.pallas_call(
        lambda *refs: totals_body(flip, *refs),
        out_shape=jax.ShapeDtypeStruct((8, ROWS, 128), BF16),
        in_specs=[pl.BlockSpec(memory_space=pltpu.SMEM)] + [pl.BlockSpec(memory_space=pltpu.VMEM)] * len(args),
        out_specs=pl.BlockSpec(memory_space=pltpu.VMEM),
        scratch_shapes=[pltpu.VMEM((3 * UNITS, TOK), BF16), pltpu.VMEM((1, D), F32)],
        compiler_params=pltpu.CompilerParams(vmem_limit_bytes=LIMIT_BYTES),
    )(me, *args)


def pair_body(me, own, came, *outs):
    x, h = lax.rem(me[0] // 2, 4), me[0] // 8
    for g in range(2):
        for d in range(4):
            i = g * 4 + lax.rem(x + d, 4)
            outs[d][g] = (own[i, :CUT].astype(F32) + came[i, :CUT].astype(F32)).astype(BF16)
    for d in range(2):
        for k in range(4):
            i = lax.rem(h + d, 2) * 4 + k
            outs[4 + d][k] = (own[i, CUT:].astype(F32) + came[i, CUT:].astype(F32)).astype(BF16)


def cross_body(me, keep, one, two, three, near, far, stay_ref, go_ref, *outs):
    x, h = lax.rem(me[0] // 2, 4), me[0] // 8

    def total(g):
        return keep[g].astype(F32) + one[g].astype(F32) + two[g].astype(F32) + three[g].astype(F32)

    stay_ref[...] = total(h)
    go_ref[...] = total(1 - h).astype(BF16)
    for d in range(4):
        i = lax.rem(x + d, 4)
        outs[d][...] = (near[i].astype(F32) + far[i].astype(F32)).astype(BF16)


def last_body(stay, came, a, b, c, d, gate_ref, up_ref, down_ref, gain_ref):
    top = (stay[...] + came[...].astype(F32)) * (1.0 / 16.0)
    total = jnp.concatenate([top, summed((a, b, c, d)) * (1.0 / 16.0)], axis=0)
    gate_ref[...] = total[:UNITS].T
    up_ref[...] = total[UNITS : 2 * UNITS].T
    down_ref[...] = total[2 * UNITS : 3 * UNITS]
    gain_ref[...] = total[3 * UNITS : 3 * UNITS + 1]


def client_perm(dh, dx, dc):
    return [
        (h * 8 + x * 2 + c, ((h + dh) % 2) * 8 + ((x + dx) % 4) * 2 + (c + dc) % 2)
        for h in range(2)
        for x in range(4)
        for c in range(2)
    ]


def along_client(array, dh, dx):
    return lax.ppermute(array, "client", client_perm(dh, dx, 0))


def along_y(array, d):
    pairs = [(y * 4 + z, (y ^ d) * 4 + z) for y in range(4) for z in range(4)]
    return lax.ppermute(array, "tp", pairs)


def along_z(array, d):
    pairs = [(y * 4 + z, y * 4 + (z ^ d)) for y in range(4) for z in range(4)]
    return lax.ppermute(array, "tp", pairs)


def to_all(array, axis):
    return lax.all_to_all(array, axis, 0, 0, tiled=True)


def on_device(inputs, targets, norm_gain, gate_weight, up_weight, down_weight, overflow):
    mine = lax.axis_index("tp").reshape(1)
    me = lax.axis_index("client").reshape(1)
    flags = overflow.reshape(STEPS)
    gain = norm_gain.reshape(1, D)
    gain_total = jnp.zeros((1, D), F32)
    weights = tuple(in_vmem(me, (gate_weight, up_weight, down_weight)))
    row = ((1, D), F32)
    made = [((TOK, D), BF16), ((TOK, 2 * UNITS), F32), ((TOK, UNITS), BF16)] + [((BLOCK, D), BF16)] * 4
    past, factors, arrived, diff = [], [], None, None
    for step in range(STEPS):
        flat = [r for p in past for r in p]
        if step == 0:
            scaled, normed, act, hidden, *parts = call(
                first_body, [((TOK, D), F32)] + made, (inputs[0], gain) + weights, (mine,)
            )
        else:
            body = lambda *refs, step=step: next_body(step, *refs)
            factor, gain, gain_total, normed, act, hidden, *parts = call(
                body,
                [((8, 128), F32), row, row] + made,
                (arrived, gain, gain_total, scaled) + weights + tuple(flat + factors),
                (mine,),
            )
            factors = factors + [factor]
        block = ((BLOCK, D), BF16)
        square = ((TOK, TOK), F32)
        ahead = call(ahead_body, [square, square, ((TOK, 2 * UNITS), F32)], (normed, act, hidden))
        if step == STEPS - 1:
            before = early((*flat, *factors))
        (rows,) = call(row_body, [block], (parts[0], *[along_y(parts[d], d) for d in (2, 3, 1)]))
        came = [along_z(rows, d) for d in (1, 2, 3)]
        if step == 0:
            error, diff = call(first_error_body, [block, ((BLOCK, D), F32)], (rows, *came, inputs[0], targets[0]), (mine,))
        else:
            done = (before,) if step == STEPS - 1 else ()
            (error,) = call(error_body, [block], (rows, *came, diff, *done))
        one, three, two = [along_y(error, d) for d in (1, 3, 2)]
        errors = (error, one, three, two)
        body = lambda *refs, step=step: back_body(step, *refs)
        error, grads, pay = call(
            body,
            [((TOK, D), BF16), ((TOK, 2 * UNITS), BF16), ((16, 8, 384), BF16)],
            errors + weights + (scaled, *ahead) + tuple(flat + factors),
            (flags, mine),
        )
        arrived = to_all(pay, "tp")
        past = past + [(normed, grads, hidden, error)]

    args = (arrived, gain_total, before, *past[-1])
    other = totals(1, me, args)
    came = lax.ppermute(other, "client", client_perm(0, 0, 1))
    own = totals(0, me, args)
    low = ROWS - CUT
    outs = [((2, CUT, 128), BF16)] * 4 + [((4, low, 128), BF16)] * 2
    keep, one, two, three, near, far = call(pair_body, outs, (own, came), (me,))
    far = along_client(far, 1, 0)
    moved = [along_client(a, 0, d) for d, a in ((1, one), (2, two), (3, three))]
    outs = [((CUT, 128), F32), ((CUT, 128), BF16)] + [((low, 128), BF16)] * 4
    stay, go, kept, one, two, three = call(cross_body, outs, (keep, *moved, near, far), (me,))
    go = along_client(go, 1, 0)
    moved = [along_client(a, 0, d) for d, a in ((1, one), (2, two), (3, three))]
    gate, up, down, gains = call(
        last_body,
        [((128, UNITS), F32), ((128, UNITS), F32), ((UNITS, 128), F32), ((1, 128), F32)],
        (stay, go, kept, *moved),
    )
    return gate, up, down, gains.reshape(128)


def solution(mesh):
    placed = (
        P("client", None, None),
        P("client", None, None),
        P(),
        P(None, "tp"),
        P(None, "tp"),
        P("tp", None),
        P("client", None, "tp"),
    )
    return jax.shard_map(
        on_device,
        mesh=mesh,
        in_specs=placed,
        out_specs=(P("client", "tp"), P("client", "tp"), P("tp", "client"), P("client")),
        check_vma=False,
    )
```

```python
import math

import jax
import jax.numpy as jnp
from jax import lax
from jax.experimental import pallas as pl
from jax.experimental.pallas import tpu as pltpu
from jax.sharding import PartitionSpec as P

D = 2048
FF = 4096
STEPS = 3
RATE = 0.005
LIMIT = 0.5 * math.sqrt(3.0 * D * FF)
TOK = 128
UNITS = 256
WIDE = 512
BLOCK = 32
LIMIT_BYTES = 20 * 1024 * 1024
FIRST_BYTES = 50 * 1024 * 1024
ROWS = 3 * UNITS + 16
CUT = 448


BF16 = jnp.bfloat16
F32 = jnp.float32


def dot_nn(a, b):
    return jnp.dot(a, b, preferred_element_type=F32)


def dot_nt(a, b):
    return lax.dot_general(a, b, (((1,), (1,)), ((), ())), preferred_element_type=F32)


def call(body, outs, args, scalars=()):
    return pl.pallas_call(
        body,
        out_shape=tuple(jax.ShapeDtypeStruct(s, d) for s, d in outs),
        in_specs=[pl.BlockSpec(memory_space=pltpu.SMEM)] * len(scalars)
        + [pl.BlockSpec(memory_space=pltpu.VMEM)] * len(args),
        out_specs=tuple(pl.BlockSpec(memory_space=pltpu.VMEM) for _ in outs),
        compiler_params=pltpu.CompilerParams(vmem_limit_bytes=LIMIT_BYTES),
    )(*scalars, *args)


def token_block(i):
    return pl.ds(pl.multiple_of(i * BLOCK, BLOCK), BLOCK)


def forward(y, normed, wg, wu, down, past, coefs, act_ref, hid_ref, *part_refs):
    gate = dot_nn(normed, wg[...])
    up = dot_nn(normed, wu[...])
    for (n, g, h, e), a in zip(past, coefs):
        k = (dot_nt(normed, n[...]) * a).astype(BF16)
        gate = gate - dot_nn(k, g[:, :UNITS])
        up = up - dot_nn(k, g[:, UNITS:])
    act_ref[:, :UNITS] = gate
    act_ref[:, UNITS:] = up
    hidden = (gate * jax.nn.sigmoid(gate) * up).astype(BF16)
    hid_ref[...] = hidden
    turned = jnp.concatenate([hid_ref[token_block(y ^ d)] for d in range(4)], axis=0)
    grams = [(dot_nt(turned, h[...]) * a).astype(BF16) for (n, g, h, e), a in zip(past, coefs)]
    for c in range(0, D, WIDE):
        share = dot_nn(turned, down[:, c : c + WIDE])
        for k, (n, g, h, e) in zip(grams, past):
            share = share - dot_nn(k, e[:, c : c + WIDE])
        for d in range(4):
            part_refs[d][:, c : c + WIDE] = share[d * BLOCK : (d + 1) * BLOCK].astype(BF16)


def weights_body(me, wg, wu, down, wg_ref, wu_ref, down_ref, sems):
    moves = [(wg, wg_ref), (wu, wu_ref), (down, down_ref)]
    moves = [pltpu.make_async_copy(a, b, sems.at[i]) for i, (a, b) in enumerate(moves)]
    for m in moves:
        m.start()
    for m in moves:
        m.wait()


def in_vmem(me, weights):
    vmem, far = pl.BlockSpec(memory_space=pltpu.VMEM), pl.BlockSpec(memory_space=pltpu.HBM)
    return pl.pallas_call(
        weights_body,
        out_shape=tuple(jax.ShapeDtypeStruct(w.shape, w.dtype) for w in weights),
        in_specs=[pl.BlockSpec(memory_space=pltpu.SMEM), far, far, far],
        out_specs=(vmem, vmem, vmem),
        scratch_shapes=[pltpu.SemaphoreType.DMA((3,))],
        compiler_params=pltpu.CompilerParams(vmem_limit_bytes=FIRST_BYTES),
    )(me, *weights)


def first_body(mine, x, gain, wg, wu, down, scaled_ref, norm_ref, act_ref, hid_ref, *part_refs):
    activ = x[...].astype(F32)
    scaled = activ * lax.rsqrt(jnp.mean(activ * activ, axis=-1, keepdims=True) + 1e-05)
    scaled_ref[...] = scaled
    normed = (scaled * gain[...]).astype(BF16)
    norm_ref[...] = normed
    forward(mine[0] // 4, normed, wg, wu, down, (), (), act_ref, hid_ref, *part_refs)


def sums_of(arrived):
    total = arrived[0].astype(F32)
    for i in range(1, 16):
        total = total + arrived[i].astype(F32)
    grad_gain = jnp.concatenate([total[r : r + 1, :256] for r in range(8)], axis=1)
    squares = jnp.sum(jnp.sum(total[0:3, 256:], axis=0, keepdims=True), axis=1, keepdims=True)
    squares = squares + jnp.sum(grad_gain * grad_gain, axis=1, keepdims=True)
    flagged = total[3:4, 256:257]
    norm = jnp.sqrt(squares + 1e-06)
    factor = jnp.where(flagged < 0.5, LIMIT / jnp.maximum(norm, LIMIT), 0.0)
    return grad_gain, factor


def next_body(step, mine, *refs):
    arrived, gain, gain_total, scaled, wg, wu, down = refs[:7]
    at = 7
    past = [refs[at + 4 * j : at + 4 * j + 4] for j in range(step)]
    at += 4 * step
    old = refs[at : at + step - 1]
    at += step - 1
    factor_ref, gain_ref, total_ref, norm_ref, act_ref, hid_ref = refs[at : at + 6]
    part_refs = refs[at + 6 :]
    grad_gain, factor = sums_of(arrived)
    factor_ref[...] = jnp.broadcast_to(factor, (8, 128))
    new_gain = gain[...] - RATE * factor * grad_gain
    gain_ref[...] = new_gain
    total_ref[...] = gain_total[...] + factor * grad_gain
    normed = (scaled[...] * new_gain).astype(BF16)
    norm_ref[...] = normed
    coefs = [RATE * r[0:1, 0:1] for r in old] + [RATE * factor]
    forward(mine[0] // 4, normed, wg, wu, down, past, coefs, act_ref, hid_ref, *part_refs)


def summed(refs):
    total = refs[0][...].astype(F32)
    for r in refs[1:]:
        total = total + r[...].astype(F32)
    return total


def row_body(*refs):
    refs[-1][...] = summed(refs[:-1]).astype(BF16)


def first_error_body(mine, a, b, c, d, x, t, out_ref, diff_ref):
    rows = token_block(mine[0] // 4)
    diff = x[rows].astype(F32) - t[rows].astype(F32)
    diff_ref[...] = diff
    out_ref[...] = (summed((a, b, c, d)) + diff).astype(BF16)


def error_body(a, b, c, d, diff, *rest):
    out_ref = rest[-1]
    out_ref[...] = (summed((a, b, c, d)) + diff[...]).astype(BF16)


def pieces(value):
    first = value.astype(BF16)
    rest = value - first.astype(F32)
    second = rest.astype(BF16)
    third = (rest - second.astype(F32)).astype(BF16)
    return [first.astype(F32), second.astype(F32), third.astype(F32)]


def ahead_body(normed, act, hidden, nn_ref, hh_ref, slope_ref):
    nn_ref[...] = dot_nt(normed[...], normed[...])
    hh_ref[...] = dot_nt(hidden[...], hidden[...])
    gate, up = act[:, :UNITS], act[:, UNITS:]
    sig = jax.nn.sigmoid(gate)
    slope_ref[:, :UNITS] = up * (sig * (1.0 + gate * (1.0 - sig)))
    slope_ref[:, UNITS:] = gate * sig


def back_body(step, flags, mine, *refs):
    errors, (wg, wu, down, scaled, nn, hh, slope) = refs[:4], refs[4:11]
    at = 11
    past = [refs[at + 4 * j : at + 4 * j + 4] for j in range(step)]
    at += 4 * step
    coefs = [RATE * r[0:1, 0:1] for r in refs[at : at + step]]
    at += step
    err_ref, grad_ref, pay_ref = refs[at:]
    for d, came in zip((0, 1, 3, 2), errors):
        err_ref[token_block((mine[0] // 4) ^ d)] = came[...]
    err = err_ref[...]
    grad_hidden = dot_nt(err, down[...])
    for (n, g, h, e), a in zip(past, coefs):
        k = (dot_nt(err, e[...]) * a).astype(BF16)
        grad_hidden = grad_hidden - dot_nn(k, h[...])
    g_gate = (grad_hidden * slope[:, :UNITS]).astype(BF16)
    g_up = (grad_hidden * slope[:, UNITS:]).astype(BF16)
    grad_ref[:, :UNITS] = g_gate
    grad_ref[:, UNITS:] = g_up
    grads = jnp.concatenate([g_gate, g_up], axis=1)
    grams = [(dot_nt(grads, g[...]) * a).astype(BF16) for (n, g, h, e), a in zip(past, coefs)]
    heads = []
    for c in range(0, D, WIDE):
        grad_normed = dot_nt(g_gate, wg[c : c + WIDE]) + dot_nt(g_up, wu[c : c + WIDE])
        for k, (n, g, h, e) in zip(grams, past):
            grad_normed = grad_normed - dot_nn(k, n[:, c : c + WIDE])
        part = jnp.sum(grad_normed * scaled[:, c : c + WIDE], axis=0, keepdims=True)
        heads += [part[:, i : i + 256] for i in range(0, WIDE, 256)]
    square = nn[...] * dot_nt(grads, grads) + dot_nt(err, err) * hh[...]
    square = jnp.sum(square, axis=0, keepdims=True)
    flag = jnp.full((1, 128), flags[step].astype(F32))
    tail = jnp.concatenate(pieces(square) + [flag, jnp.zeros((4, 128), F32)], axis=0)
    head = jnp.concatenate(heads, axis=0)
    packed = jnp.concatenate([head, tail], axis=1).astype(BF16)
    for i in range(16):
        pay_ref[i] = packed


def early_body(*refs):
    past = [refs[4 * j : 4 * j + 4] for j in range(STEPS - 1)]
    factors = refs[4 * (STEPS - 1) : 5 * (STEPS - 1)]
    out_ref, left = refs[5 * (STEPS - 1) :]
    for j, ((n, g, h, e), r) in enumerate(zip(past, factors)):
        f = r[0:1, 0:1]
        left[: 2 * UNITS, j * TOK : (j + 1) * TOK] = (g[...].astype(F32) * f).T.astype(BF16)
        left[2 * UNITS :, j * TOK : (j + 1) * TOK] = (h[...].astype(F32) * f).T.astype(BF16)

    def two_blocks(i, carry):
        col = pl.ds(pl.multiple_of(i * 256, 256), 256)
        rows = jnp.concatenate([p[0][:, col] for p in past], axis=0)
        errs = jnp.concatenate([p[3][:, col] for p in past], axis=0)
        top, low = dot_nn(left[: 2 * UNITS], rows), dot_nn(left[2 * UNITS :], errs)
        for k in range(2):
            out_ref[2 * i + k, : 2 * UNITS] = top[:, k * 128 : (k + 1) * 128]
            out_ref[2 * i + k, 2 * UNITS :] = low[:, k * 128 : (k + 1) * 128]
        return carry

    lax.fori_loop(0, 8, two_blocks, 0)


def early(args):
    vmem = pl.BlockSpec(memory_space=pltpu.VMEM)
    return pl.pallas_call(
        early_body,
        out_shape=jax.ShapeDtypeStruct((16, 3 * UNITS, 128), F32),
        in_specs=[vmem] * len(args),
        out_specs=vmem,
        scratch_shapes=[pltpu.VMEM((3 * UNITS, (STEPS - 1) * TOK), BF16)],
        compiler_params=pltpu.CompilerParams(vmem_limit_bytes=LIMIT_BYTES),
    )(*args)


def totals_body(flip, me, arrived, gain_total, before, n, g, h, e, out_ref, left, gain_row):
    grad_gain, factor = sums_of(arrived)
    gain_row[...] = gain_total[...] + factor * grad_gain
    left[: 2 * UNITS] = (g[...].astype(F32) * factor).T.astype(BF16)
    left[2 * UNITS :] = (h[...].astype(F32) * factor).T.astype(BF16)
    w = lax.rem(me[0] + flip, 2)
    for b in range(8):
        i = 2 * b + w
        col = pl.ds(pl.multiple_of(i * 128, 128), 128)
        top = before[i, : 2 * UNITS] + dot_nn(left[: 2 * UNITS], n[:, col])
        low = before[i, 2 * UNITS :] + dot_nn(left[2 * UNITS :], e[:, col])
        out_ref[b, : 2 * UNITS] = top.astype(BF16)
        out_ref[b, 2 * UNITS : 3 * UNITS] = low.astype(BF16)
        out_ref[b, 3 * UNITS :] = jnp.broadcast_to(gain_row[:, col], (16, 128)).astype(BF16)


def totals(flip, me, args):
    return pl.pallas_call(
        lambda *refs: totals_body(flip, *refs),
        out_shape=jax.ShapeDtypeStruct((8, ROWS, 128), BF16),
        in_specs=[pl.BlockSpec(memory_space=pltpu.SMEM)] + [pl.BlockSpec(memory_space=pltpu.VMEM)] * len(args),
        out_specs=pl.BlockSpec(memory_space=pltpu.VMEM),
        scratch_shapes=[pltpu.VMEM((3 * UNITS, TOK), BF16), pltpu.VMEM((1, D), F32)],
        compiler_params=pltpu.CompilerParams(vmem_limit_bytes=LIMIT_BYTES),
    )(me, *args)


def pair_body(me, own, came, *outs):
    x, h = lax.rem(me[0] // 2, 4), me[0] // 8
    for g in range(2):
        for d in range(4):
            i = g * 4 + lax.rem(x + d, 4)
            outs[d][g] = (own[i, :CUT].astype(F32) + came[i, :CUT].astype(F32)).astype(BF16)
    for d in range(2):
        for k in range(4):
            i = lax.rem(h + d, 2) * 4 + k
            outs[4 + d][k] = (own[i, CUT:].astype(F32) + came[i, CUT:].astype(F32)).astype(BF16)


def cross_body(me, keep, one, two, three, near, far, stay_ref, go_ref, *outs):
    x, h = lax.rem(me[0] // 2, 4), me[0] // 8

    def total(g):
        return keep[g].astype(F32) + one[g].astype(F32) + two[g].astype(F32) + three[g].astype(F32)

    stay_ref[...] = total(h)
    go_ref[...] = total(1 - h).astype(BF16)
    for d in range(4):
        i = lax.rem(x + d, 4)
        outs[d][...] = (near[i].astype(F32) + far[i].astype(F32)).astype(BF16)


def last_body(stay, came, a, b, c, d, gate_ref, up_ref, down_ref, gain_ref):
    top = (stay[...] + came[...].astype(F32)) * (1.0 / 16.0)
    total = jnp.concatenate([top, summed((a, b, c, d)) * (1.0 / 16.0)], axis=0)
    gate_ref[...] = total[:UNITS].T
    up_ref[...] = total[UNITS : 2 * UNITS].T
    down_ref[...] = total[2 * UNITS : 3 * UNITS]
    gain_ref[...] = total[3 * UNITS : 3 * UNITS + 1]


def client_perm(dh, dx, dc):
    return [
        (h * 8 + x * 2 + c, ((h + dh) % 2) * 8 + ((x + dx) % 4) * 2 + (c + dc) % 2)
        for h in range(2)
        for x in range(4)
        for c in range(2)
    ]


def along_client(array, dh, dx):
    return lax.ppermute(array, "client", client_perm(dh, dx, 0))


def along_y(array, d):
    pairs = [(y * 4 + z, (y ^ d) * 4 + z) for y in range(4) for z in range(4)]
    return lax.ppermute(array, "tp", pairs)


def along_z(array, d):
    pairs = [(y * 4 + z, y * 4 + (z ^ d)) for y in range(4) for z in range(4)]
    return lax.ppermute(array, "tp", pairs)


def to_all(array, axis):
    return lax.all_to_all(array, axis, 0, 0, tiled=True)


def on_device(inputs, targets, norm_gain, gate_weight, up_weight, down_weight, overflow):
    mine = lax.axis_index("tp").reshape(1)
    me = lax.axis_index("client").reshape(1)
    flags = overflow.reshape(STEPS)
    gain = norm_gain.reshape(1, D)
    gain_total = jnp.zeros((1, D), F32)
    weights = tuple(in_vmem(me, (gate_weight, up_weight, down_weight)))
    row = ((1, D), F32)
    made = [((TOK, D), BF16), ((TOK, 2 * UNITS), F32), ((TOK, UNITS), BF16)] + [((BLOCK, D), BF16)] * 4
    past, factors, arrived, diff = [], [], None, None
    for step in range(STEPS):
        flat = [r for p in past for r in p]
        if step == 0:
            scaled, normed, act, hidden, *parts = call(
                first_body, [((TOK, D), F32)] + made, (inputs[0], gain) + weights, (mine,)
            )
        else:
            body = lambda *refs, step=step: next_body(step, *refs)
            factor, gain, gain_total, normed, act, hidden, *parts = call(
                body,
                [((8, 128), F32), row, row] + made,
                (arrived, gain, gain_total, scaled) + weights + tuple(flat + factors),
                (mine,),
            )
            factors = factors + [factor]
        block = ((BLOCK, D), BF16)
        square = ((TOK, TOK), F32)
        ahead = call(ahead_body, [square, square, ((TOK, 2 * UNITS), F32)], (normed, act, hidden))
        if step == STEPS - 1:
            before = early((*flat, *factors))
        (rows,) = call(row_body, [block], (parts[0], *[along_y(parts[d], d) for d in (2, 3, 1)]))
        came = [along_z(rows, d) for d in (1, 2, 3)]
        if step == 0:
            error, diff = call(first_error_body, [block, ((BLOCK, D), F32)], (rows, *came, inputs[0], targets[0]), (mine,))
        else:
            done = (before,) if step == STEPS - 1 else ()
            (error,) = call(error_body, [block], (rows, *came, diff, *done))
        one, three, two = [along_y(error, d) for d in (1, 3, 2)]
        errors = (error, one, three, two)
        body = lambda *refs, step=step: back_body(step, *refs)
        error, grads, pay = call(
            body,
            [((TOK, D), BF16), ((TOK, 2 * UNITS), BF16), ((16, 8, 384), BF16)],
            errors + weights + (scaled, *ahead) + tuple(flat + factors),
            (flags, mine),
        )
        arrived = to_all(pay, "tp")
        past = past + [(normed, grads, hidden, error)]

    args = (arrived, gain_total, before, *past[-1])
    other = totals(1, me, args)
    came = lax.ppermute(other, "client", client_perm(0, 0, 1))
    own = totals(0, me, args)
    low = ROWS - CUT
    outs = [((2, CUT, 128), BF16)] * 4 + [((4, low, 128), BF16)] * 2
    keep, one, two, three, near, far = call(pair_body, outs, (own, came), (me,))
    far = along_client(far, 1, 0)
    moved = [along_client(a, 0, d) for d, a in ((1, one), (2, two), (3, three))]
    outs = [((CUT, 128), F32), ((CUT, 128), BF16)] + [((low, 128), BF16)] * 4
    stay, go, kept, one, two, three = call(cross_body, outs, (keep, *moved, near, far), (me,))
    go = along_client(go, 1, 0)
    moved = [along_client(a, 0, d) for d, a in ((1, one), (2, two), (3, three))]
    gate, up, down, gains = call(
        last_body,
        [((128, UNITS), F32), ((128, UNITS), F32), ((UNITS, 128), F32), ((1, 128), F32)],
        (stay, go, kept, *moved),
    )
    return gate, up, down, gains.reshape(128)


def solution(mesh):
    placed = (
        P("client", None, None),
        P("client", None, None),
        P(),
        P(None, "tp"),
        P(None, "tp"),
        P("tp", None),
        P("client", None, "tp"),
    )
    return jax.shard_map(
        on_device,
        mesh=mesh,
        in_specs=placed,
        out_specs=(P("client", "tp"), P("client", "tp"), P("tp", "client"), P("client")),
        check_vma=False,
    )
```

```python
import math

import jax
import jax.numpy as jnp
from jax import lax
from jax.experimental import pallas as pl
from jax.experimental.pallas import tpu as pltpu
from jax.sharding import PartitionSpec as P

D = 2048
FF = 4096
STEPS = 3
RATE = 0.005
LIMIT = 0.5 * math.sqrt(3.0 * D * FF)
TOK = 128
UNITS = 256
WIDE = 1024
BLOCK = 32
LIMIT_BYTES = 20 * 1024 * 1024
FIRST_BYTES = 50 * 1024 * 1024
ROWS = 3 * UNITS + 16
CUT = 448


BF16 = jnp.bfloat16
F32 = jnp.float32


def dot_nn(a, b):
    return jnp.dot(a, b, preferred_element_type=F32)


def dot_nt(a, b):
    return lax.dot_general(a, b, (((1,), (1,)), ((), ())), preferred_element_type=F32)


def call(body, outs, args, scalars=()):
    return pl.pallas_call(
        body,
        out_shape=tuple(jax.ShapeDtypeStruct(s, d) for s, d in outs),
        in_specs=[pl.BlockSpec(memory_space=pltpu.SMEM)] * len(scalars)
        + [pl.BlockSpec(memory_space=pltpu.VMEM)] * len(args),
        out_specs=tuple(pl.BlockSpec(memory_space=pltpu.VMEM) for _ in outs),
        compiler_params=pltpu.CompilerParams(vmem_limit_bytes=LIMIT_BYTES),
    )(*scalars, *args)


def token_block(i):
    return pl.ds(pl.multiple_of(i * BLOCK, BLOCK), BLOCK)


def forward(y, normed, wg, wu, down, past, coefs, act_ref, hid_ref, *part_refs):
    gate = dot_nn(normed, wg[...])
    up = dot_nn(normed, wu[...])
    for (n, g, h, e), a in zip(past, coefs):
        k = (dot_nt(normed, n[...]) * a).astype(BF16)
        gate = gate - dot_nn(k, g[:, :UNITS])
        up = up - dot_nn(k, g[:, UNITS:])
    act_ref[:, :UNITS] = gate
    act_ref[:, UNITS:] = up
    hidden = (gate * jax.nn.sigmoid(gate) * up).astype(BF16)
    hid_ref[...] = hidden
    turned = jnp.concatenate([hid_ref[token_block(y ^ d)] for d in range(4)], axis=0)
    grams = [(dot_nt(turned, h[...]) * a).astype(BF16) for (n, g, h, e), a in zip(past, coefs)]
    for c in range(0, D, WIDE):
        share = dot_nn(turned, down[:, c : c + WIDE])
        for k, (n, g, h, e) in zip(grams, past):
            share = share - dot_nn(k, e[:, c : c + WIDE])
        for d in range(4):
            part_refs[d][:, c : c + WIDE] = share[d * BLOCK : (d + 1) * BLOCK].astype(BF16)


def weights_body(me, wg, wu, down, wg_ref, wu_ref, down_ref, sems):
    moves = [(wg, wg_ref), (wu, wu_ref), (down, down_ref)]
    moves = [pltpu.make_async_copy(a, b, sems.at[i]) for i, (a, b) in enumerate(moves)]
    for m in moves:
        m.start()
    for m in moves:
        m.wait()


def in_vmem(me, weights):
    vmem, far = pl.BlockSpec(memory_space=pltpu.VMEM), pl.BlockSpec(memory_space=pltpu.HBM)
    return pl.pallas_call(
        weights_body,
        out_shape=tuple(jax.ShapeDtypeStruct(w.shape, w.dtype) for w in weights),
        in_specs=[pl.BlockSpec(memory_space=pltpu.SMEM), far, far, far],
        out_specs=(vmem, vmem, vmem),
        scratch_shapes=[pltpu.SemaphoreType.DMA((3,))],
        compiler_params=pltpu.CompilerParams(vmem_limit_bytes=FIRST_BYTES),
    )(me, *weights)


def first_body(mine, x, gain, wg, wu, down, scaled_ref, norm_ref, act_ref, hid_ref, *part_refs):
    activ = x[...].astype(F32)
    scaled = activ * lax.rsqrt(jnp.mean(activ * activ, axis=-1, keepdims=True) + 1e-05)
    scaled_ref[...] = scaled
    normed = (scaled * gain[...]).astype(BF16)
    norm_ref[...] = normed
    forward(mine[0] // 4, normed, wg, wu, down, (), (), act_ref, hid_ref, *part_refs)


def sums_of(arrived):
    total = arrived[0].astype(F32)
    for i in range(1, 16):
        total = total + arrived[i].astype(F32)
    grad_gain = jnp.concatenate([total[r : r + 1, :256] for r in range(8)], axis=1)
    squares = jnp.sum(jnp.sum(total[0:3, 256:], axis=0, keepdims=True), axis=1, keepdims=True)
    squares = squares + jnp.sum(grad_gain * grad_gain, axis=1, keepdims=True)
    flagged = total[3:4, 256:257]
    norm = jnp.sqrt(squares + 1e-06)
    factor = jnp.where(flagged < 0.5, LIMIT / jnp.maximum(norm, LIMIT), 0.0)
    return grad_gain, factor


def next_body(step, mine, *refs):
    arrived, gain, gain_total, scaled, wg, wu, down = refs[:7]
    at = 7
    past = [refs[at + 4 * j : at + 4 * j + 4] for j in range(step)]
    at += 4 * step
    old = refs[at : at + step - 1]
    at += step - 1
    factor_ref, gain_ref, total_ref, norm_ref, act_ref, hid_ref = refs[at : at + 6]
    part_refs = refs[at + 6 :]
    grad_gain, factor = sums_of(arrived)
    factor_ref[...] = jnp.broadcast_to(factor, (8, 128))
    new_gain = gain[...] - RATE * factor * grad_gain
    gain_ref[...] = new_gain
    total_ref[...] = gain_total[...] + factor * grad_gain
    normed = (scaled[...] * new_gain).astype(BF16)
    norm_ref[...] = normed
    coefs = [RATE * r[0:1, 0:1] for r in old] + [RATE * factor]
    forward(mine[0] // 4, normed, wg, wu, down, past, coefs, act_ref, hid_ref, *part_refs)


def summed(refs):
    total = refs[0][...].astype(F32)
    for r in refs[1:]:
        total = total + r[...].astype(F32)
    return total


def row_body(*refs):
    refs[-1][...] = summed(refs[:-1]).astype(BF16)


def first_error_body(mine, a, b, c, d, x, t, out_ref, diff_ref):
    rows = token_block(mine[0] // 4)
    diff = x[rows].astype(F32) - t[rows].astype(F32)
    diff_ref[...] = diff
    out_ref[...] = (summed((a, b, c, d)) + diff).astype(BF16)


def error_body(a, b, c, d, diff, *rest):
    out_ref = rest[-1]
    out_ref[...] = (summed((a, b, c, d)) + diff[...]).astype(BF16)


def pieces(value):
    first = value.astype(BF16)
    rest = value - first.astype(F32)
    second = rest.astype(BF16)
    third = (rest - second.astype(F32)).astype(BF16)
    return [first.astype(F32), second.astype(F32), third.astype(F32)]


def ahead_body(normed, act, hidden, nn_ref, hh_ref, slope_ref):
    nn_ref[...] = dot_nt(normed[...], normed[...])
    hh_ref[...] = dot_nt(hidden[...], hidden[...])
    gate, up = act[:, :UNITS], act[:, UNITS:]
    sig = jax.nn.sigmoid(gate)
    slope_ref[:, :UNITS] = up * (sig * (1.0 + gate * (1.0 - sig)))
    slope_ref[:, UNITS:] = gate * sig


def back_body(step, flags, mine, *refs):
    errors, (wg, wu, down, scaled, nn, hh, slope) = refs[:4], refs[4:11]
    at = 11
    past = [refs[at + 4 * j : at + 4 * j + 4] for j in range(step)]
    at += 4 * step
    coefs = [RATE * r[0:1, 0:1] for r in refs[at : at + step]]
    at += step
    err_ref, grad_ref, pay_ref = refs[at:]
    for d, came in zip((0, 1, 3, 2), errors):
        err_ref[token_block((mine[0] // 4) ^ d)] = came[...]
    err = err_ref[...]
    grad_hidden = dot_nt(err, down[...])
    for (n, g, h, e), a in zip(past, coefs):
        k = (dot_nt(err, e[...]) * a).astype(BF16)
        grad_hidden = grad_hidden - dot_nn(k, h[...])
    g_gate = (grad_hidden * slope[:, :UNITS]).astype(BF16)
    g_up = (grad_hidden * slope[:, UNITS:]).astype(BF16)
    grad_ref[:, :UNITS] = g_gate
    grad_ref[:, UNITS:] = g_up
    grads = jnp.concatenate([g_gate, g_up], axis=1)
    grams = [(dot_nt(grads, g[...]) * a).astype(BF16) for (n, g, h, e), a in zip(past, coefs)]
    heads = []
    for c in range(0, D, WIDE):
        grad_normed = dot_nt(g_gate, wg[c : c + WIDE]) + dot_nt(g_up, wu[c : c + WIDE])
        for k, (n, g, h, e) in zip(grams, past):
            grad_normed = grad_normed - dot_nn(k, n[:, c : c + WIDE])
        part = jnp.sum(grad_normed * scaled[:, c : c + WIDE], axis=0, keepdims=True)
        heads += [part[:, i : i + 256] for i in range(0, WIDE, 256)]
    square = nn[...] * dot_nt(grads, grads) + dot_nt(err, err) * hh[...]
    square = jnp.sum(square, axis=0, keepdims=True)
    flag = jnp.full((1, 128), flags[step].astype(F32))
    tail = jnp.concatenate(pieces(square) + [flag, jnp.zeros((4, 128), F32)], axis=0)
    head = jnp.concatenate(heads, axis=0)
    packed = jnp.concatenate([head, tail], axis=1).astype(BF16)
    for i in range(16):
        pay_ref[i] = packed


def early_body(*refs):
    past = [refs[4 * j : 4 * j + 4] for j in range(STEPS - 1)]
    factors = refs[4 * (STEPS - 1) : 5 * (STEPS - 1)]
    out_ref, left = refs[5 * (STEPS - 1) :]
    for j, ((n, g, h, e), r) in enumerate(zip(past, factors)):
        f = r[0:1, 0:1]
        left[: 2 * UNITS, j * TOK : (j + 1) * TOK] = (g[...].astype(F32) * f).T.astype(BF16)
        left[2 * UNITS :, j * TOK : (j + 1) * TOK] = (h[...].astype(F32) * f).T.astype(BF16)

    def two_blocks(i, carry):
        col = pl.ds(pl.multiple_of(i * 256, 256), 256)
        rows = jnp.concatenate([p[0][:, col] for p in past], axis=0)
        errs = jnp.concatenate([p[3][:, col] for p in past], axis=0)
        top, low = dot_nn(left[: 2 * UNITS], rows), dot_nn(left[2 * UNITS :], errs)
        for k in range(2):
            out_ref[2 * i + k, : 2 * UNITS] = top[:, k * 128 : (k + 1) * 128]
            out_ref[2 * i + k, 2 * UNITS :] = low[:, k * 128 : (k + 1) * 128]
        return carry

    lax.fori_loop(0, 8, two_blocks, 0)


def early(args):
    vmem = pl.BlockSpec(memory_space=pltpu.VMEM)
    return pl.pallas_call(
        early_body,
        out_shape=jax.ShapeDtypeStruct((16, 3 * UNITS, 128), F32),
        in_specs=[vmem] * len(args),
        out_specs=vmem,
        scratch_shapes=[pltpu.VMEM((3 * UNITS, (STEPS - 1) * TOK), BF16)],
        compiler_params=pltpu.CompilerParams(vmem_limit_bytes=LIMIT_BYTES),
    )(*args)


def totals_body(flip, me, arrived, gain_total, before, n, g, h, e, out_ref, left, gain_row):
    grad_gain, factor = sums_of(arrived)
    gain_row[...] = gain_total[...] + factor * grad_gain
    left[: 2 * UNITS] = (g[...].astype(F32) * factor).T.astype(BF16)
    left[2 * UNITS :] = (h[...].astype(F32) * factor).T.astype(BF16)
    w = lax.rem(me[0] + flip, 2)
    for b in range(8):
        i = 2 * b + w
        col = pl.ds(pl.multiple_of(i * 128, 128), 128)
        top = before[i, : 2 * UNITS] + dot_nn(left[: 2 * UNITS], n[:, col])
        low = before[i, 2 * UNITS :] + dot_nn(left[2 * UNITS :], e[:, col])
        out_ref[b, : 2 * UNITS] = top.astype(BF16)
        out_ref[b, 2 * UNITS : 3 * UNITS] = low.astype(BF16)
        out_ref[b, 3 * UNITS :] = jnp.broadcast_to(gain_row[:, col], (16, 128)).astype(BF16)


def totals(flip, me, args):
    return pl.pallas_call(
        lambda *refs: totals_body(flip, *refs),
        out_shape=jax.ShapeDtypeStruct((8, ROWS, 128), BF16),
        in_specs=[pl.BlockSpec(memory_space=pltpu.SMEM)] + [pl.BlockSpec(memory_space=pltpu.VMEM)] * len(args),
        out_specs=pl.BlockSpec(memory_space=pltpu.VMEM),
        scratch_shapes=[pltpu.VMEM((3 * UNITS, TOK), BF16), pltpu.VMEM((1, D), F32)],
        compiler_params=pltpu.CompilerParams(vmem_limit_bytes=LIMIT_BYTES),
    )(me, *args)


def pair_body(me, own, came, *outs):
    x, h = lax.rem(me[0] // 2, 4), me[0] // 8
    for g in range(2):
        for d in range(4):
            i = g * 4 + lax.rem(x + d, 4)
            outs[d][g] = (own[i, :CUT].astype(F32) + came[i, :CUT].astype(F32)).astype(BF16)
    for d in range(2):
        for k in range(4):
            i = lax.rem(h + d, 2) * 4 + k
            outs[4 + d][k] = (own[i, CUT:].astype(F32) + came[i, CUT:].astype(F32)).astype(BF16)


def cross_body(me, keep, one, two, three, near, far, stay_ref, go_ref, *outs):
    x, h = lax.rem(me[0] // 2, 4), me[0] // 8

    def total(g):
        return keep[g].astype(F32) + one[g].astype(F32) + two[g].astype(F32) + three[g].astype(F32)

    stay_ref[...] = total(h)
    go_ref[...] = total(1 - h).astype(BF16)
    for d in range(4):
        i = lax.rem(x + d, 4)
        outs[d][...] = (near[i].astype(F32) + far[i].astype(F32)).astype(BF16)


def last_body(stay, came, a, b, c, d, gate_ref, up_ref, down_ref, gain_ref):
    top = (stay[...] + came[...].astype(F32)) * (1.0 / 16.0)
    total = jnp.concatenate([top, summed((a, b, c, d)) * (1.0 / 16.0)], axis=0)
    gate_ref[...] = total[:UNITS].T
    up_ref[...] = total[UNITS : 2 * UNITS].T
    down_ref[...] = total[2 * UNITS : 3 * UNITS]
    gain_ref[...] = total[3 * UNITS : 3 * UNITS + 1]


def client_perm(dh, dx, dc):
    return [
        (h * 8 + x * 2 + c, ((h + dh) % 2) * 8 + ((x + dx) % 4) * 2 + (c + dc) % 2)
        for h in range(2)
        for x in range(4)
        for c in range(2)
    ]


def along_client(array, dh, dx):
    return lax.ppermute(array, "client", client_perm(dh, dx, 0))


def along_y(array, d):
    pairs = [(y * 4 + z, (y ^ d) * 4 + z) for y in range(4) for z in range(4)]
    return lax.ppermute(array, "tp", pairs)


def along_z(array, d):
    pairs = [(y * 4 + z, y * 4 + (z ^ d)) for y in range(4) for z in range(4)]
    return lax.ppermute(array, "tp", pairs)


def to_all(array, axis):
    return lax.all_to_all(array, axis, 0, 0, tiled=True)


def on_device(inputs, targets, norm_gain, gate_weight, up_weight, down_weight, overflow):
    mine = lax.axis_index("tp").reshape(1)
    me = lax.axis_index("client").reshape(1)
    flags = overflow.reshape(STEPS)
    gain = norm_gain.reshape(1, D)
    gain_total = jnp.zeros((1, D), F32)
    weights = tuple(in_vmem(me, (gate_weight, up_weight, down_weight)))
    row = ((1, D), F32)
    made = [((TOK, D), BF16), ((TOK, 2 * UNITS), F32), ((TOK, UNITS), BF16)] + [((BLOCK, D), BF16)] * 4
    past, factors, arrived, diff = [], [], None, None
    for step in range(STEPS):
        flat = [r for p in past for r in p]
        if step == 0:
            scaled, normed, act, hidden, *parts = call(
                first_body, [((TOK, D), F32)] + made, (inputs[0], gain) + weights, (mine,)
            )
        else:
            body = lambda *refs, step=step: next_body(step, *refs)
            factor, gain, gain_total, normed, act, hidden, *parts = call(
                body,
                [((8, 128), F32), row, row] + made,
                (arrived, gain, gain_total, scaled) + weights + tuple(flat + factors),
                (mine,),
            )
            factors = factors + [factor]
        block = ((BLOCK, D), BF16)
        square = ((TOK, TOK), F32)
        ahead = call(ahead_body, [square, square, ((TOK, 2 * UNITS), F32)], (normed, act, hidden))
        if step == STEPS - 1:
            before = early((*flat, *factors))
        (rows,) = call(row_body, [block], (parts[0], *[along_y(parts[d], d) for d in (2, 3, 1)]))
        came = [along_z(rows, d) for d in (1, 2, 3)]
        if step == 0:
            error, diff = call(first_error_body, [block, ((BLOCK, D), F32)], (rows, *came, inputs[0], targets[0]), (mine,))
        else:
            done = (before,) if step == STEPS - 1 else ()
            (error,) = call(error_body, [block], (rows, *came, diff, *done))
        one, three, two = [along_y(error, d) for d in (1, 3, 2)]
        errors = (error, one, three, two)
        body = lambda *refs, step=step: back_body(step, *refs)
        error, grads, pay = call(
            body,
            [((TOK, D), BF16), ((TOK, 2 * UNITS), BF16), ((16, 8, 384), BF16)],
            errors + weights + (scaled, *ahead) + tuple(flat + factors),
            (flags, mine),
        )
        arrived = to_all(pay, "tp")
        past = past + [(normed, grads, hidden, error)]

    args = (arrived, gain_total, before, *past[-1])
    other = totals(1, me, args)
    came = lax.ppermute(other, "client", client_perm(0, 0, 1))
    own = totals(0, me, args)
    low = ROWS - CUT
    outs = [((2, CUT, 128), BF16)] * 4 + [((4, low, 128), BF16)] * 2
    keep, one, two, three, near, far = call(pair_body, outs, (own, came), (me,))
    far = along_client(far, 1, 0)
    moved = [along_client(a, 0, d) for d, a in ((1, one), (2, two), (3, three))]
    outs = [((CUT, 128), F32), ((CUT, 128), BF16)] + [((low, 128), BF16)] * 4
    stay, go, kept, one, two, three = call(cross_body, outs, (keep, *moved, near, far), (me,))
    go = along_client(go, 1, 0)
    moved = [along_client(a, 0, d) for d, a in ((1, one), (2, two), (3, three))]
    gate, up, down, gains = call(
        last_body,
        [((128, UNITS), F32), ((128, UNITS), F32), ((UNITS, 128), F32), ((1, 128), F32)],
        (stay, go, kept, *moved),
    )
    return gate, up, down, gains.reshape(128)


def solution(mesh):
    placed = (
        P("client", None, None),
        P("client", None, None),
        P(),
        P(None, "tp"),
        P(None, "tp"),
        P("tp", None),
        P("client", None, "tp"),
    )
    return jax.shard_map(
        on_device,
        mesh=mesh,
        in_specs=placed,
        out_specs=(P("client", "tp"), P("client", "tp"), P("tp", "client"), P("client")),
        check_vma=False,
    )
```
